32 devices in a mesh: rows: 16 (over z, y, x), feat: 2 (over core).
Axes of the slice: x: 2, y: 2, z: 4, core: 2. Of those that a mesh axis runs over, the one named last changes fastest.
Arguments:
- queries: bfloat16 [1024, 128], P('rows', 'feat'), may hold values from -6 to 6
- corpus: bfloat16 [524288, 128], P(('rows', 'feat')), as said below
- candidates: int32 [1024, 100], P(('rows', 'feat')), may hold values from 0 to 524287, as said below
- threshold: int32 [1024], replicated, may hold values from 100 to 199, as said below
Outputs:
- exceed: float32 [1024], P(('rows', 'feat'))
- candidate_scores: float32 [1024, 100], P(('rows', 'feat'))
The draws below stay inside these ranges and needn't reach their ends.
Inputs may be any that keep to these rules, and one draw needn't show every extreme that they name: Passage ids. Of the 3200 candidates of one device's queries (aligned blocks of 32 rows), at most 100 lie in the 16384 passages of any one device, and exactly 100 in some device's. `corpus`: passage embeddings of order one or smaller; their scale differs between passages. Some query has threshold 100 and some 199.
All inputs are finite; a program needn't handle non-finite values.
Results may differ from the reference program's by a relative error of at most 0.00035.
Values may be sent and summed in bfloat16 or wider, within the bound.
A program may use at most 64 MiB of HBM per device.

```python
import jax
import jax.numpy as jnp
from jax import lax

DIM = 128
NQ = 1024
NCAND = 100
ROWS_DEV = 16384
SHARDS = 32
NPASS = 524288
NQ_DEV = 32


def draw_corpus(key, part):
    blocks_count = NPASS // ROWS_DEV
    block_scale = jnp.exp(jax.random.uniform(jax.random.fold_in(key, 11), (blocks_count,), jnp.float32, jnp.log(0.3), jnp.log(3.0)))
    row_scale = jax.random.uniform(jax.random.fold_in(key, 12), (NPASS,), jnp.float32, 0.7, 1.3)
    base = jax.random.normal(jax.random.fold_in(key, 13), (NPASS, DIM), jnp.float32)
    scale = jnp.repeat(block_scale, ROWS_DEV) * row_scale
    return (base * DIM ** (-0.5) * scale[:, None]).astype(jnp.bfloat16)


def draw_candidates(key, part):
    total = NQ_DEV * NCAND

    def one_source(source):
        source_key = jax.random.fold_in(key, source)
        order = jax.random.permutation(jax.random.fold_in(source_key, 1), total)
        target = order % SHARDS
        offset = jax.random.randint(jax.random.fold_in(source_key, 2), (total,), 0, ROWS_DEV)
        return (target * ROWS_DEV + offset).reshape(NQ_DEV, NCAND)
    sources = jnp.arange(NQ // NQ_DEV, dtype=jnp.int32)
    return jax.vmap(one_source)(sources).reshape(NQ, NCAND).astype(jnp.int32)


def draw_threshold(key, part):
    values = jax.random.randint(jax.random.fold_in(key, 21), (NQ,), 100, 200).astype(jnp.int32)
    order = jax.random.permutation(jax.random.fold_in(key, 22), NQ)
    values = values.at[order[0]].set(100)
    values = values.at[order[1]].set(199)
    return values.astype(jnp.int32)


def block_levels(key, dims, pieces, low, top_value):
    factor_of = 1.0
    for dim, blocks in pieces:
        heights = jax.random.uniform(jax.random.fold_in(jax.random.fold_in(key, 6), dim), (blocks,), jnp.float32, low / len(pieces), top_value / len(pieces))
        factor_of = factor_of * jnp.repeat(jnp.exp(heights), dims[dim] // blocks).reshape((-1,) + (1,) * (len(dims) - 1 - dim))
    return factor_of


def centred(own_key, shape, deviation, reach, shards=(), held_as=jnp.bfloat16):
    result = deviation * jax.random.normal(own_key, shape, jnp.float32)
    if shards:
        result = result * block_levels(own_key, shape, shards, -0.22, 0.18)
    return jnp.clip(result, -reach, reach).astype(held_as)


def setup_inputs(seed: int = 0) -> dict:
    key_list = jax.random.split(jax.random.key(seed), 5)
    queries = centred(key_list[0], (NQ, DIM), 1.0, 6.0, ((0, 16), (1, 2)))
    corpus = draw_corpus(jax.random.fold_in(key_list[4], 71), 0)
    candidates = draw_candidates(jax.random.fold_in(key_list[4], 71), 0)
    threshold = draw_threshold(jax.random.fold_in(key_list[4], 71), 0)
    return {"queries": queries, "corpus": corpus, "candidates": candidates, "threshold": threshold}


def reference(queries, corpus, candidates, threshold):
    cutoff = threshold.astype(jnp.float32) * 0.01
    blocks = corpus.reshape(NPASS // ROWS_DEV, ROWS_DEV, DIM)

    def visit(total, block):
        scores = lax.dot_general(queries, block, (((1,), (1,)), ((), ())), preferred_element_type=jnp.float32)
        return total + jnp.sum(jnp.maximum(scores - cutoff[:, None], 0.0), axis=1), None

    total, _ = lax.scan(visit, jnp.zeros((NQ,), jnp.float32), blocks)
    exceed = total * (8.0 / NPASS)
    flat_ids = candidates.reshape(-1).astype(jnp.int32)
    picked = corpus[flat_ids].astype(jnp.float32).reshape(NQ, NCAND, DIM)
    candidate_scores = jnp.einsum("qkd,qd->qk", picked, queries.astype(jnp.float32), precision=lax.Precision.HIGHEST)
    return exceed, candidate_scores
```

```python
import functools

import jax
import jax.numpy as jnp
from jax import lax
from jax.experimental import pallas as pl
from jax.experimental.pallas import tpu as pltpu
from jax.sharding import PartitionSpec as P

LANES = 128
TILE = 256
BLOCK = 512
MESH = pl.DeviceIdType.MESH


def bulk_wait(ref, sem):
    pltpu.make_async_copy(ref, ref, sem).wait()


def kernel(
    n, nf, npass_all, capacity,
    q_ref, thr_ref, cand_ref, corpus_ref,
    mass_out, ans_out,
    corpus_v, corpus_f, q_pack, q_in, q_full, cand_pad, ranks, places,
    ids_out, ids_in, ids_sm, rows_v, vals_out, vals_in, mass_rows, mass_in,
    load_sem, sm_sem, q_send, q_recv, ids_send, ids_recv, vals_send, vals_recv, mass_send, mass_recv,
):
    rows_dev, width = corpus_v.shape
    owned, per_query = cand_ref.shape
    nq = q_full.shape[0]
    half = q_ref.shape[1]
    tiles = nq // TILE
    dpt = TILE // owned
    me = lax.axis_index("rows") * nf + lax.axis_index("feat")
    my_tile = me // dpt
    my_j = me % dpt
    id_bits = rows_dev.bit_length() - 1

    load = pltpu.make_async_copy(corpus_ref, corpus_v, load_sem)
    load.start()

    def tile_at(i):
        return (my_tile + i) % tiles

    def peers(i, act):
        def step(j, carry):
            act(tile_at(i) * dpt + (my_j + j) % dpt)
            return carry
        lax.fori_loop(1 if i == 0 else 0, dpt, step, 0)

    def where_is(d):
        return (d // nf, d % nf)

    barrier = pltpu.get_barrier_semaphore()
    for i in range(tiles):
        peers(i, lambda d: pl.semaphore_signal(
            barrier, inc=1, device_id=where_is(d), device_id_type=MESH))

    q_local = q_ref[...].astype(jnp.float32)
    mine = jnp.concatenate([q_local[:owned], q_local[owned:]], axis=1).astype(jnp.bfloat16)
    q_pack[...] = mine
    q_in[me] = mine

    cand_pad[...] = jnp.full(cand_pad.shape, -1, jnp.int32)
    cand_pad[:, :per_query] = cand_ref[...]
    cand = cand_pad[...]
    target = lax.shift_right_arithmetic(cand, jnp.int32(id_bits))
    local = jnp.bitwise_and(cand, jnp.int32(rows_dev - 1))
    low = jnp.bitwise_and(local, jnp.int32(LANES - 1)).astype(jnp.float32)
    high = lax.shift_right_arithmetic(local, jnp.int32(7)).astype(jnp.float32)
    dest = lax.broadcasted_iota(jnp.int32, (n, LANES), 0)
    hot = [jnp.where(target[q:q + 1] == dest, 1.0, 0.0) for q in range(owned)]
    row_i = lax.broadcasted_iota(jnp.int32, (LANES, 2 * LANES), 0)
    col_i = lax.broadcasted_iota(jnp.int32, (LANES, 2 * LANES), 1)
    upper = jnp.where((row_i < col_i) | (col_i >= LANES), 1.0, 0.0).astype(jnp.bfloat16)
    counts = jnp.dot(
        jnp.concatenate(hot, axis=0).astype(jnp.bfloat16), upper, preferred_element_type=jnp.float32)
    base = jnp.zeros((n, LANES), jnp.float32)
    slot = lax.broadcasted_iota(jnp.int32, (LANES, LANES), 0).astype(jnp.float32)
    fields = []
    for q in range(owned):
        block = counts[q * n:(q + 1) * n]
        rank = jnp.sum(hot[q] * (block[:, :LANES] + base), axis=0, keepdims=True)
        base = base + block[:, LANES:]
        places[:, q * LANES:(q + 1) * LANES] = jnp.where(rank == slot, 1.0, 0.0).astype(jnp.bfloat16)
        fields.append(jnp.concatenate(
            [hot[q] * low[q:q + 1], hot[q] * high[q:q + 1], hot[q] * float(q)], axis=0
        ).astype(jnp.bfloat16))
    sorted_fields = lax.dot_general(
        jnp.concatenate(fields, axis=1), places[...], (((1,), (1,)), ((), ())),
        preferred_element_type=jnp.float32)
    packed = (
        sorted_fields[:n] + sorted_fields[n:2 * n] * float(LANES) + sorted_fields[2 * n:] * float(rows_dev)
    ).astype(jnp.int32)
    for t in range(n):
        ids_out[t] = packed[t:t + 1]

    pl.semaphore_wait(barrier, n - 1)

    for i in range(tiles):
        def send_queries(d):
            pltpu.make_async_remote_copy(
                src_ref=q_pack, dst_ref=q_in.at[me], send_sem=q_send, recv_sem=q_recv.at[my_tile],
                device_id=where_is(d), device_id_type=MESH).start()
        peers(i, send_queries)
    for i in range(tiles):
        def send_ids(d):
            pltpu.make_async_remote_copy(
                src_ref=ids_out.at[d], dst_ref=ids_in.at[me], send_sem=ids_send, recv_sem=ids_recv,
                device_id=where_is(d), device_id_type=MESH).start()
        peers(i, send_ids)
    ids_in[me] = ids_out[me]

    load.wait()

    def widen(b, carry):
        at = pl.ds(pl.multiple_of(b * BLOCK, BLOCK), BLOCK)
        corpus_f[at, :] = corpus_v[at, :].astype(jnp.float32)
        return carry
    lax.fori_loop(0, rows_dev // BLOCK, widen, 0)

    left = lax.broadcasted_iota(jnp.int32, (owned, LANES), 1) < half
    to_smem = pltpu.make_async_copy(ids_in, ids_sm, sm_sem)
    blocks = rows_dev // BLOCK
    for i in range(tiles):
        tile = tile_at(i)
        if i == 0:
            bulk_wait(q_in.at[pl.ds(0, dpt - 1)], q_recv.at[tile])
        else:
            bulk_wait(q_in.at[pl.ds(0, dpt)], q_recv.at[tile])
        parts = []
        for g in range(dpt // 2):
            f0 = q_in[tile * dpt + 2 * g].astype(jnp.float32)
            f1 = q_in[tile * dpt + 2 * g + 1].astype(jnp.float32)
            parts.append(jnp.where(left, f0, pltpu.roll(f1, half, 1)))
            parts.append(jnp.where(left, pltpu.roll(f0, half, 1), f1))
        asked = jnp.concatenate(parts, axis=0)
        start = pl.multiple_of(tile * TILE, TILE)
        q_full[pl.ds(start, TILE), :] = asked.astype(jnp.bfloat16)
        weights = asked.T.astype(jnp.bfloat16)
        cutoff = thr_ref[:, pl.ds(start, TILE)].astype(jnp.float32) * 0.01
        if i == tiles - 2:
            bulk_wait(ids_in.at[pl.ds(0, n - 1)], ids_recv)
            to_smem.start()
            to_smem.wait()

        def sweep(b, acc):
            at = pl.ds(pl.multiple_of(b * BLOCK, BLOCK), BLOCK)
            scores = jnp.dot(corpus_v[at, :], weights, preferred_element_type=jnp.float32)
            over = jnp.maximum(scores - cutoff, 0.0)
            if i == tiles - 2:
                for r in range(capacity):
                    p = jnp.bitwise_and(ids_sm[b, 0, r], rows_dev - 1)
                    rows_v[b, pl.ds(r, 1), :] = corpus_f[pl.ds(p, 1), :]
            if i == tiles - 1:
                pairs = lax.dot_general(
                    q_full[pl.ds(pl.multiple_of(b * owned, owned), owned), :],
                    rows_v[b].astype(jnp.bfloat16),
                    (((1,), (1,)), ((), ())), preferred_element_type=jnp.float32)
                who = lax.shift_right_arithmetic(ids_in[b], jnp.int32(id_bits))
                mask = (who == lax.broadcasted_iota(jnp.int32, (owned, LANES), 0)) & (
                    lax.broadcasted_iota(jnp.int32, (owned, LANES), 1) < capacity)
                vals_out[b] = jnp.sum(jnp.where(mask, pairs, 0.0), axis=0, keepdims=True)
            return acc + jnp.sum(over.reshape(BLOCK // 8, 8, TILE), axis=0)

        acc = lax.fori_loop(0, blocks, sweep, jnp.zeros((8, TILE), jnp.float32))
        total = jnp.sum(acc, axis=0, keepdims=True)
        for h in range(TILE // LANES):
            mass_rows[tile * (TILE // LANES) + h] = total[:, h * LANES:(h + 1) * LANES]

        def send_mass(d):
            pltpu.make_async_remote_copy(
                src_ref=mass_rows.at[d * owned // LANES], dst_ref=mass_in.at[me],
                send_sem=mass_send, recv_sem=mass_recv,
                device_id=where_is(d), device_id_type=MESH).start()
        peers(i, send_mass)
        if i == 0:
            mass_in[me] = mass_rows[me * owned // LANES]

    for i in range(tiles):
        def send_vals(d):
            pltpu.make_async_remote_copy(
                src_ref=vals_out.at[d], dst_ref=vals_in.at[me], send_sem=vals_send, recv_sem=vals_recv,
                device_id=where_is(d), device_id_type=MESH).start()
        peers(i, send_vals)
    vals_in[me] = vals_out[me]

    bulk_wait(vals_in.at[pl.ds(0, n - 1)], vals_recv)
    values = jnp.concatenate([vals_in[t] for t in range(n)], axis=0)
    top = values.astype(jnp.bfloat16)
    rest = values - top.astype(jnp.float32)
    mid = rest.astype(jnp.bfloat16)
    last = (rest - mid.astype(jnp.float32)).astype(jnp.bfloat16)
    pieces = jnp.concatenate([top, mid, last], axis=0)
    cand = cand_pad[...]
    target = lax.shift_right_arithmetic(cand, jnp.int32(id_bits))
    for q in range(owned):
        spread = jnp.dot(
            pieces, places[:, q * LANES:(q + 1) * LANES], preferred_element_type=jnp.float32)
        spread = (spread[2 * n:] + spread[n:2 * n]) + spread[:n]
        ans_out[q:q + 1, :] = jnp.sum(
            jnp.where(target[q:q + 1] == dest, spread, 0.0), axis=0, keepdims=True)

    bulk_wait(mass_in.at[pl.ds(0, n - 1)], mass_recv)
    mass = mass_in[0]
    for t in range(1, n):
        mass = mass + mass_in[t]
    mass = mass * (8.0 / npass_all)
    per_row = LANES // owned
    result = mass
    for u in range(1, per_row):
        result = jnp.where(me % per_row == u, pltpu.roll(mass, LANES - u * owned, 1), result)
    mass_out[...] = result

    bulk_wait(q_in.at[pl.ds(0, n - 1)], q_send)
    bulk_wait(ids_in.at[pl.ds(0, n - 1)], ids_send)
    bulk_wait(vals_in.at[pl.ds(0, n - 1)], vals_send)
    bulk_wait(mass_in.at[pl.ds(0, n - 1)], mass_send)


def fused_body(n, nf, queries, corpus, candidates, threshold):
    rows_dev, width = corpus.shape
    owned, per_query = candidates.shape
    nq = n * owned
    capacity = (owned * per_query + n - 1) // n
    vmem = pl.BlockSpec(memory_space=pltpu.VMEM)
    mass, answers = pl.pallas_call(
        functools.partial(kernel, n, nf, rows_dev * n, capacity),
        out_shape=(
            jax.ShapeDtypeStruct((1, LANES), jnp.float32),
            jax.ShapeDtypeStruct((owned, LANES), jnp.float32),
        ),
        in_specs=[vmem, vmem, vmem, pl.BlockSpec(memory_space=pl.ANY)],
        out_specs=(vmem, vmem),
        scratch_shapes=[
            pltpu.VMEM((rows_dev, width), jnp.bfloat16),
            pltpu.VMEM((rows_dev, width), jnp.float32),
            pltpu.VMEM((owned, LANES), jnp.bfloat16),
            pltpu.VMEM((n, owned, LANES), jnp.bfloat16),
            pltpu.VMEM((nq, LANES), jnp.bfloat16),
            pltpu.VMEM((owned, LANES), jnp.int32),
            pltpu.VMEM((owned, LANES), jnp.float32),
            pltpu.VMEM((LANES, owned * LANES), jnp.bfloat16),
            pltpu.VMEM((n, 1, LANES), jnp.int32),
            pltpu.VMEM((n, 1, LANES), jnp.int32),
            pltpu.SMEM((n, 1, LANES), jnp.int32),
            pltpu.VMEM((n, LANES, LANES), jnp.float32),
            pltpu.VMEM((n, 1, LANES), jnp.float32),
            pltpu.VMEM((n, 1, LANES), jnp.float32),
            pltpu.VMEM((nq // LANES, 1, LANES), jnp.float32),
            pltpu.VMEM((n, 1, LANES), jnp.float32),
            pltpu.SemaphoreType.DMA,
            pltpu.SemaphoreType.DMA,
            pltpu.SemaphoreType.DMA,
            pltpu.SemaphoreType.DMA((nq // TILE,)),
            pltpu.SemaphoreType.DMA,
            pltpu.SemaphoreType.DMA,
            pltpu.SemaphoreType.DMA,
            pltpu.SemaphoreType.DMA,
            pltpu.SemaphoreType.DMA,
            pltpu.SemaphoreType.DMA,
        ],
        compiler_params=pltpu.CompilerParams(
            collective_id=0, has_side_effects=True, vmem_limit_bytes=48 * 1024 * 1024),
    )(queries, threshold.reshape(1, nq), candidates, corpus)
    return mass[0, :owned], answers[:, :per_query]


def plain_body(queries, corpus, candidates, threshold):
    rows_dev = corpus.shape[0]
    width = corpus.shape[1]
    shards = lax.axis_size("rows") * lax.axis_size("feat")
    owned_queries = candidates.shape[0]
    per_query = candidates.shape[1]
    npass_all = rows_dev * shards
    cutoff = threshold.astype(jnp.float32) * 0.01
    owner = lax.axis_index(("rows", "feat"))
    full_rows = lax.all_gather(queries, "feat", axis=1, tiled=True)
    whole = lax.all_gather(full_rows, "rows", axis=0, tiled=True)
    query_count = whole.shape[0]
    block = 2048
    corpus_blocks = corpus.reshape(rows_dev // block, block, width)

    def visit(total, block_rows):
        scores = lax.dot_general(
            whole, block_rows, (((1,), (1,)), ((), ())), preferred_element_type=jnp.float32
        )
        return (total + jnp.sum(jnp.maximum(scores - cutoff[:, None], 0.0), axis=1), None)

    total, _ = lax.scan(visit, jnp.zeros((query_count,), jnp.float32), corpus_blocks)
    flat_ids = candidates.reshape(-1)
    total_ids = flat_ids.shape[0]
    capacity = (total_ids + shards - 1) // shards
    target = flat_ids // rows_dev
    onehot = (target[:, None] == jnp.arange(shards, dtype=jnp.int32)[None, :]).astype(jnp.int32)
    before = jnp.cumsum(onehot, axis=0) - onehot
    rank = jnp.sum(before * onehot, axis=1)
    query_ids = owner * owned_queries + jnp.arange(total_ids, dtype=jnp.int32) // per_query
    fields = jnp.stack([flat_ids - target * rows_dev, query_ids], axis=1)
    send_both = jnp.zeros((shards, capacity, 2), jnp.int32).at[target, rank].set(fields)
    n_rows = lax.axis_size("rows")
    n_feat = lax.axis_size("feat")
    received = lax.all_to_all(
        lax.all_to_all(
            send_both.reshape(n_rows, n_feat, capacity * 2),
            "rows",
            split_axis=0,
            concat_axis=0,
            tiled=True,
        ),
        "feat",
        split_axis=1,
        concat_axis=1,
        tiled=True,
    )
    received = received.reshape(shards * capacity, 2)
    picked = corpus[received[:, 0]]
    asked = whole[received[:, 1]]
    values = jnp.einsum("kd,kd->k", picked, asked, preferred_element_type=jnp.float32).reshape(
        n_rows, n_feat, capacity
    )
    partials = total.reshape(n_rows, n_feat, owned_queries)
    answers, mass_parts = (
        lax.all_to_all(
            lax.all_to_all(values, "rows", split_axis=0, concat_axis=0, tiled=True),
            "feat",
            split_axis=1,
            concat_axis=1,
            tiled=True,
        ),
        lax.all_to_all(
            lax.all_to_all(partials, "rows", split_axis=0, concat_axis=0, tiled=True),
            "feat",
            split_axis=1,
            concat_axis=1,
            tiled=True,
        ),
    )
    exceed = jnp.sum(mass_parts, axis=(0, 1)) * (8.0 / npass_all)
    candidate_scores = answers.reshape(shards, capacity)[target, rank].reshape(
        owned_queries, per_query
    )
    return (exceed, candidate_scores)


def body(queries, corpus, candidates, threshold):
    nf = lax.axis_size("feat")
    n = lax.axis_size("rows") * nf
    rows_dev, width = corpus.shape
    owned, per_query = candidates.shape
    capacity = (owned * per_query + n - 1) // n
    fits = (
        nf == 2
        and width == LANES
        and queries.shape == (2 * owned, LANES // 2)
        and owned % 32 == 0
        and LANES % owned == 0
        and per_query <= LANES
        and capacity <= LANES
        and n % 8 == 0
        and (n * owned) % TILE == 0
        and n * owned >= 2 * TILE
        and rows_dev == n * BLOCK
        and rows_dev & (rows_dev - 1) == 0
    )
    if fits:
        return fused_body(n, nf, queries, corpus, candidates, threshold)
    return plain_body(queries, corpus, candidates, threshold)


def solution(mesh):
    return jax.shard_map(
        body,
        mesh=mesh,
        in_specs=(P("rows", "feat"), P(("rows", "feat"), None), P(("rows", "feat"), None), P()),
        out_specs=(P(("rows", "feat")), P(("rows", "feat"), None)),
        check_vma=False,
    )
```

```python
import functools

import jax
import jax.numpy as jnp
from jax import lax
from jax.experimental import pallas as pl
from jax.experimental.pallas import tpu as pltpu
from jax.sharding import PartitionSpec as P

LANES = 128
TILE = 256
BLOCK = 4096
STEP = 512
MESH = pl.DeviceIdType.MESH


def bulk_wait(ref, sem):
    pltpu.make_async_copy(ref, ref, sem).wait()


def kernel(
    n, nf, npass_all, capacity,
    q_hbm, thr_hbm, cand_hbm, corpus_ref,
    mass_out, ans_out,
    q_ref, thr_ref, cand_ref, corpus_v, corpus_f, q_pack, q_in, q_full, cand_pad, places,
    ids_out, ids_in, ids_at, ids_sm, rows_v, vals_out, vals_in, mass_rows, mass_in,
    small_sem, load_sem, sm_sem, q_send, q_recv, ids_send, ids_recv, vals_send, vals_recv, mass_send, mass_recv,
):
    rows_dev, width = corpus_v.shape
    owned, per_query = cand_ref.shape
    nq = q_full.shape[0]
    half = q_ref.shape[1]
    tiles = nq // TILE
    dpt = TILE // owned
    me = lax.axis_index("rows") * nf + lax.axis_index("feat")
    my_tile = me // dpt
    my_j = me % dpt
    id_bits = rows_dev.bit_length() - 1

    load = pltpu.make_async_copy(corpus_ref, corpus_v, load_sem)
    small = [
        pltpu.make_async_copy(src, dst, small_sem.at[k])
        for k, (src, dst) in enumerate(((q_hbm, q_ref), (cand_hbm, cand_ref), (thr_hbm, thr_ref)))]
    for copy in small:
        copy.start()
    load.start()

    def tile_at(i):
        return (my_tile + i) % tiles

    def peers(i, act):
        def step(j, carry):
            act(tile_at(i) * dpt + (my_j + j) % dpt)
            return carry
        lax.fori_loop(1 if i == 0 else 0, dpt, step, 0)

    def where_is(d):
        return (d // nf, d % nf)

    barrier = pltpu.get_barrier_semaphore()
    for i in range(tiles):
        peers(i, lambda d: pl.semaphore_signal(
            barrier, inc=1, device_id=where_is(d), device_id_type=MESH))

    for copy in small:
        copy.wait()
    q_local = q_ref[...].astype(jnp.float32)
    mine = jnp.concatenate([q_local[:owned], q_local[owned:]], axis=1).astype(jnp.bfloat16)
    q_pack[...] = mine
    q_in[me] = mine

    cand_pad[...] = jnp.full(cand_pad.shape, -1, jnp.int32)
    cand_pad[:, :per_query] = cand_ref[...]
    cand = cand_pad[...]
    target = lax.shift_right_arithmetic(cand, jnp.int32(id_bits))
    local = jnp.bitwise_and(cand, jnp.int32(rows_dev - 1))
    low = jnp.bitwise_and(local, jnp.int32(LANES - 1)).astype(jnp.float32)
    high = lax.shift_right_arithmetic(local, jnp.int32(7)).astype(jnp.float32)
    dest = lax.broadcasted_iota(jnp.int32, (n, LANES), 0)
    hot = [jnp.where(target[q:q + 1] == dest, 1.0, 0.0) for q in range(owned)]
    row_i = lax.broadcasted_iota(jnp.int32, (LANES, 2 * LANES), 0)
    col_i = lax.broadcasted_iota(jnp.int32, (LANES, 2 * LANES), 1)
    upper = jnp.where((row_i < col_i) | (col_i >= LANES), 1.0, 0.0).astype(jnp.bfloat16)
    counts = jnp.dot(
        jnp.concatenate(hot, axis=0).astype(jnp.bfloat16), upper, preferred_element_type=jnp.float32)
    base = jnp.zeros((n, LANES), jnp.float32)
    slot = lax.broadcasted_iota(jnp.int32, (LANES, LANES), 0).astype(jnp.float32)
    fields = []
    for q in range(owned):
        block = counts[q * n:(q + 1) * n]
        rank = jnp.sum(hot[q] * (block[:, :LANES] + base), axis=0, keepdims=True)
        base = base + block[:, LANES:]
        places[:, q * LANES:(q + 1) * LANES] = jnp.where(rank == slot, 1.0, 0.0).astype(jnp.bfloat16)
        fields.append(jnp.concatenate(
            [hot[q] * low[q:q + 1], hot[q] * high[q:q + 1], hot[q] * float(q)], axis=0
        ).astype(jnp.bfloat16))
    sorted_fields = lax.dot_general(
        jnp.concatenate(fields, axis=1), places[...], (((1,), (1,)), ((), ())),
        preferred_element_type=jnp.float32)
    packed = (
        sorted_fields[:n] + sorted_fields[n:2 * n] * float(LANES) + sorted_fields[2 * n:] * float(rows_dev)
    ).astype(jnp.int32)
    for t in range(n):
        ids_out[t] = packed[t:t + 1]

    pl.semaphore_wait(barrier, n - 1)

    for i in range(tiles):
        def send_queries(d):
            pltpu.make_async_remote_copy(
                src_ref=q_pack, dst_ref=q_in.at[me], send_sem=q_send, recv_sem=q_recv.at[my_tile],
                device_id=where_is(d), device_id_type=MESH).start()
        peers(i, send_queries)
    for i in range(tiles):
        def send_ids(d):
            pltpu.make_async_remote_copy(
                src_ref=ids_out.at[d], dst_ref=ids_in.at[me], send_sem=ids_send, recv_sem=ids_recv,
                device_id=where_is(d), device_id_type=MESH).start()
        peers(i, send_ids)
    ids_in[me] = ids_out[me]

    load.wait()

    def widen(b, carry):
        at = pl.ds(pl.multiple_of(b * STEP, STEP), STEP)
        corpus_f[at, :] = corpus_v[at, :].astype(jnp.float32)
        return carry
    lax.fori_loop(0, rows_dev // STEP, widen, 0)

    left = lax.broadcasted_iota(jnp.int32, (owned, LANES), 1) < half
    to_smem = pltpu.make_async_copy(ids_at, ids_sm, sm_sem)
    blocks = rows_dev // BLOCK
    part = n // (2 * blocks)

    def collect(source):
        for r in range(capacity):
            rows_v[source, pl.ds(r, 1), :] = corpus_f[pl.ds(ids_sm[source, 0, r], 1), :]

    def answer(source):
        pairs = lax.dot_general(
            q_full[pl.ds(pl.multiple_of(source * owned, owned), owned), :],
            rows_v[source].astype(jnp.bfloat16),
            (((1,), (1,)), ((), ())), preferred_element_type=jnp.float32)
        who = lax.shift_right_arithmetic(ids_in[source], jnp.int32(id_bits))
        mask = (who == lax.broadcasted_iota(jnp.int32, (owned, LANES), 0)) & (
            lax.broadcasted_iota(jnp.int32, (owned, LANES), 1) < capacity)
        vals_out[source] = jnp.sum(jnp.where(mask, pairs, 0.0), axis=0, keepdims=True)

    for i in range(tiles):
        tile = tile_at(i)
        if i == 0:
            bulk_wait(q_in.at[pl.ds(0, dpt - 1)], q_recv.at[tile])
        else:
            bulk_wait(q_in.at[pl.ds(0, dpt)], q_recv.at[tile])
        parts = []
        for g in range(dpt // 2):
            f0 = q_in[tile * dpt + 2 * g].astype(jnp.float32)
            f1 = q_in[tile * dpt + 2 * g + 1].astype(jnp.float32)
            parts.append(jnp.where(left, f0, pltpu.roll(f1, half, 1)))
            parts.append(jnp.where(left, pltpu.roll(f0, half, 1), f1))
        asked = jnp.concatenate(parts, axis=0)
        start = pl.multiple_of(tile * TILE, TILE)
        q_full[pl.ds(start, TILE), :] = asked.astype(jnp.bfloat16)
        weights = asked.T.astype(jnp.bfloat16)
        cutoff = thr_ref[:, pl.ds(start, TILE)].astype(jnp.float32) * 0.01
        if i == tiles - 2:
            bulk_wait(ids_in.at[pl.ds(0, n - 1)], ids_recv)
            ids_at[...] = jnp.bitwise_and(ids_in[...], jnp.int32(rows_dev - 1))
            to_smem.start()
            to_smem.wait()

        def sweep(b, acc):
            at = pl.ds(pl.multiple_of(b * BLOCK, BLOCK), BLOCK)
            scores = jnp.dot(corpus_v[at, :], weights, preferred_element_type=jnp.float32)
            over = jnp.maximum(scores - cutoff, 0.0)
            for k in range(part):
                if i == tiles - 2:
                    collect(b * part + k)
                if i == tiles - 1:
                    collect(n // 2 + b * part + k)
                    answer(b * part + k)
                    answer(n // 2 + jnp.maximum(b - 1, 0) * part + k)
            return acc + jnp.sum(over.reshape(BLOCK // 8, 8, TILE), axis=0)

        acc = lax.fori_loop(0, blocks, sweep, jnp.zeros((8, TILE), jnp.float32))
        total = jnp.sum(acc, axis=0, keepdims=True)
        for h in range(TILE // LANES):
            mass_rows[tile * (TILE // LANES) + h] = total[:, h * LANES:(h + 1) * LANES]

        def send_mass(d):
            pltpu.make_async_remote_copy(
                src_ref=mass_rows.at[d * owned // LANES], dst_ref=mass_in.at[me],
                send_sem=mass_send, recv_sem=mass_recv,
                device_id=where_is(d), device_id_type=MESH).start()
        peers(i, send_mass)
        if i == 0:
            mass_in[me] = mass_rows[me * owned // LANES]

    for k in range(part):
        answer(n - part + k)
    for i in range(tiles):
        def send_vals(d):
            pltpu.make_async_remote_copy(
                src_ref=vals_out.at[d], dst_ref=vals_in.at[me], send_sem=vals_send, recv_sem=vals_recv,
                device_id=where_is(d), device_id_type=MESH).start()
        peers(i, send_vals)
    vals_in[me] = vals_out[me]

    bulk_wait(vals_in.at[pl.ds(0, n - 1)], vals_recv)
    values = jnp.concatenate([vals_in[t] for t in range(n)], axis=0)
    top = values.astype(jnp.bfloat16)
    rest = values - top.astype(jnp.float32)
    mid = rest.astype(jnp.bfloat16)
    last = (rest - mid.astype(jnp.float32)).astype(jnp.bfloat16)
    pieces = jnp.concatenate([top, mid, last], axis=0)
    cand = cand_pad[...]
    target = lax.shift_right_arithmetic(cand, jnp.int32(id_bits))
    for q in range(owned):
        spread = jnp.dot(
            pieces, places[:, q * LANES:(q + 1) * LANES], preferred_element_type=jnp.float32)
        spread = (spread[2 * n:] + spread[n:2 * n]) + spread[:n]
        ans_out[q:q + 1, :] = jnp.sum(
            jnp.where(target[q:q + 1] == dest, spread, 0.0), axis=0, keepdims=True)

    bulk_wait(mass_in.at[pl.ds(0, n - 1)], mass_recv)
    mass = mass_in[0]
    for t in range(1, n):
        mass = mass + mass_in[t]
    mass = mass * (8.0 / npass_all)
    per_row = LANES // owned
    result = mass
    for u in range(1, per_row):
        result = jnp.where(me % per_row == u, pltpu.roll(mass, LANES - u * owned, 1), result)
    mass_out[...] = result

    bulk_wait(q_in.at[pl.ds(0, n - 1)], q_send)
    bulk_wait(ids_in.at[pl.ds(0, n - 1)], ids_send)
    bulk_wait(vals_in.at[pl.ds(0, n - 1)], vals_send)
    bulk_wait(mass_in.at[pl.ds(0, n - 1)], mass_send)


def fused_body(n, nf, queries, corpus, candidates, threshold):
    rows_dev, width = corpus.shape
    owned, per_query = candidates.shape
    nq = n * owned
    capacity = (owned * per_query + n - 1) // n
    vmem = pl.BlockSpec(memory_space=pltpu.VMEM)
    mass, answers = pl.pallas_call(
        functools.partial(kernel, n, nf, rows_dev * n, capacity),
        out_shape=(
            jax.ShapeDtypeStruct((1, LANES), jnp.float32),
            jax.ShapeDtypeStruct((owned, LANES), jnp.float32),
        ),
        in_specs=[pl.BlockSpec(memory_space=pl.ANY)] * 4,
        out_specs=(vmem, vmem),
        scratch_shapes=[
            pltpu.VMEM(queries.shape, jnp.bfloat16),
            pltpu.VMEM((1, nq), jnp.int32),
            pltpu.VMEM((owned, per_query), jnp.int32),
            pltpu.VMEM((rows_dev, width), jnp.bfloat16),
            pltpu.VMEM((rows_dev, width), jnp.float32),
            pltpu.VMEM((owned, LANES), jnp.bfloat16),
            pltpu.VMEM((n, owned, LANES), jnp.bfloat16),
            pltpu.VMEM((nq, LANES), jnp.bfloat16),
            pltpu.VMEM((owned, LANES), jnp.int32),
            pltpu.VMEM((LANES, owned * LANES), jnp.bfloat16),
            pltpu.VMEM((n, 1, LANES), jnp.int32),
            pltpu.VMEM((n, 1, LANES), jnp.int32),
            pltpu.VMEM((n, 1, LANES), jnp.int32),
            pltpu.SMEM((n, 1, LANES), jnp.int32),
            pltpu.VMEM((n, LANES, LANES), jnp.float32),
            pltpu.VMEM((n, 1, LANES), jnp.float32),
            pltpu.VMEM((n, 1, LANES), jnp.float32),
            pltpu.VMEM((nq // LANES, 1, LANES), jnp.float32),
            pltpu.VMEM((n, 1, LANES), jnp.float32),
            pltpu.SemaphoreType.DMA((3,)),
            pltpu.SemaphoreType.DMA,
            pltpu.SemaphoreType.DMA,
            pltpu.SemaphoreType.DMA,
            pltpu.SemaphoreType.DMA((nq // TILE,)),
            pltpu.SemaphoreType.DMA,
            pltpu.SemaphoreType.DMA,
            pltpu.SemaphoreType.DMA,
            pltpu.SemaphoreType.DMA,
            pltpu.SemaphoreType.DMA,
            pltpu.SemaphoreType.DMA,
        ],
        compiler_params=pltpu.CompilerParams(
            collective_id=0, has_side_effects=True),
    )(queries, threshold.reshape(1, nq), candidates, corpus)
    return mass[0, :owned], answers[:, :per_query]


def plain_body(queries, corpus, candidates, threshold):
    rows_dev = corpus.shape[0]
    width = corpus.shape[1]
    shards = lax.axis_size("rows") * lax.axis_size("feat")
    owned_queries = candidates.shape[0]
    per_query = candidates.shape[1]
    npass_all = rows_dev * shards
    cutoff = threshold.astype(jnp.float32) * 0.01
    owner = lax.axis_index(("rows", "feat"))
    full_rows = lax.all_gather(queries, "feat", axis=1, tiled=True)
    whole = lax.all_gather(full_rows, "rows", axis=0, tiled=True)
    query_count = whole.shape[0]
    block = 2048
    corpus_blocks = corpus.reshape(rows_dev // block, block, width)

    def visit(total, block_rows):
        scores = lax.dot_general(
            whole, block_rows, (((1,), (1,)), ((), ())), preferred_element_type=jnp.float32
        )
        return (total + jnp.sum(jnp.maximum(scores - cutoff[:, None], 0.0), axis=1), None)

    total, _ = lax.scan(visit, jnp.zeros((query_count,), jnp.float32), corpus_blocks)
    flat_ids = candidates.reshape(-1)
    total_ids = flat_ids.shape[0]
    capacity = (total_ids + shards - 1) // shards
    target = flat_ids // rows_dev
    onehot = (target[:, None] == jnp.arange(shards, dtype=jnp.int32)[None, :]).astype(jnp.int32)
    before = jnp.cumsum(onehot, axis=0) - onehot
    rank = jnp.sum(before * onehot, axis=1)
    query_ids = owner * owned_queries + jnp.arange(total_ids, dtype=jnp.int32) // per_query
    fields = jnp.stack([flat_ids - target * rows_dev, query_ids], axis=1)
    send_both = jnp.zeros((shards, capacity, 2), jnp.int32).at[target, rank].set(fields)
    n_rows = lax.axis_size("rows")
    n_feat = lax.axis_size("feat")
    received = lax.all_to_all(
        lax.all_to_all(
            send_both.reshape(n_rows, n_feat, capacity * 2),
            "rows",
            split_axis=0,
            concat_axis=0,
            tiled=True,
        ),
        "feat",
        split_axis=1,
        concat_axis=1,
        tiled=True,
    )
    received = received.reshape(shards * capacity, 2)
    picked = corpus[received[:, 0]]
    asked = whole[received[:, 1]]
    values = jnp.einsum("kd,kd->k", picked, asked, preferred_element_type=jnp.float32).reshape(
        n_rows, n_feat, capacity
    )
    partials = total.reshape(n_rows, n_feat, owned_queries)
    answers, mass_parts = (
        lax.all_to_all(
            lax.all_to_all(values, "rows", split_axis=0, concat_axis=0, tiled=True),
            "feat",
            split_axis=1,
            concat_axis=1,
            tiled=True,
        ),
        lax.all_to_all(
            lax.all_to_all(partials, "rows", split_axis=0, concat_axis=0, tiled=True),
            "feat",
            split_axis=1,
            concat_axis=1,
            tiled=True,
        ),
    )
    exceed = jnp.sum(mass_parts, axis=(0, 1)) * (8.0 / npass_all)
    candidate_scores = answers.reshape(shards, capacity)[target, rank].reshape(
        owned_queries, per_query
    )
    return (exceed, candidate_scores)


def body(queries, corpus, candidates, threshold):
    nf = lax.axis_size("feat")
    n = lax.axis_size("rows") * nf
    rows_dev, width = corpus.shape
    owned, per_query = candidates.shape
    capacity = (owned * per_query + n - 1) // n
    fits = (
        nf == 2
        and width == LANES
        and queries.shape == (2 * owned, LANES // 2)
        and owned % 32 == 0
        and LANES % owned == 0
        and per_query <= LANES
        and capacity <= LANES
        and n % 8 == 0
        and (n * owned) % TILE == 0
        and n * owned >= 2 * TILE
        and rows_dev % BLOCK == 0
        and n % (2 * (rows_dev // BLOCK)) == 0
        and rows_dev & (rows_dev - 1) == 0
    )
    if fits:
        return fused_body(n, nf, queries, corpus, candidates, threshold)
    return plain_body(queries, corpus, candidates, threshold)


def solution(mesh):
    return jax.shard_map(
        body,
        mesh=mesh,
        in_specs=(P("rows", "feat"), P(("rows", "feat"), None), P(("rows", "feat"), None), P()),
        out_specs=(P(("rows", "feat")), P(("rows", "feat"), None)),
        check_vma=False,
    )
```

```python
import functools

import jax
import jax.numpy as jnp
from jax import lax
from jax.experimental import pallas as pl
from jax.experimental.pallas import tpu as pltpu
from jax.sharding import PartitionSpec as P

LANES = 128
TILE = 256
BLOCK = 4096
STEP = 512
MESH = pl.DeviceIdType.MESH


def bulk_wait(ref, sem):
    pltpu.make_async_copy(ref, ref, sem).wait()


def kernel(
    n, nf, npass_all, capacity,
    q_hbm, thr_hbm, cand_hbm, corpus_ref,
    mass_out, ans_out,
    q_ref, thr_ref, cand_ref, corpus_v, corpus_f, q_pack, q_in, q_full, q_turned, cand_pad, places,
    ids_out, ids_in, ids_at, ids_sm, rows_v, vals_out, vals_in, mass_rows, mass_in,
    small_sem, load_sem, sm_sem, q_send, q_recv, hand_send, hand_recv, ids_send, ids_recv, vals_send, vals_recv, mass_send, mass_recv,
):
    rows_dev, width = corpus_v.shape
    owned, per_query = cand_ref.shape
    nq = q_full.shape[0]
    half = q_ref.shape[1]
    tiles = nq // TILE
    dpt = TILE // owned
    chips = n // nf
    dpc = dpt // nf
    core = lax.axis_index("feat")
    me = lax.axis_index("rows") * nf + core
    my_tile = me // dpt
    my_j = me % dpt
    id_bits = rows_dev.bit_length() - 1
    beside = my_tile + 1 - 2 * (my_tile % 2)
    order = [beside]
    for k in range(1, tiles // 2):
        order += [(my_tile + 2 * k) % tiles, (beside + 2 * k) % tiles]
    order.append(my_tile)

    load = pltpu.make_async_copy(corpus_ref, corpus_v, load_sem)
    small = [
        pltpu.make_async_copy(src, dst, small_sem.at[k])
        for k, (src, dst) in enumerate(((q_hbm, q_ref), (cand_hbm, cand_ref), (thr_hbm, thr_ref)))]
    for copy in small:
        copy.start()
    load.start()

    def peers(i, act):
        def step(j, carry):
            act(order[i] * dpt + (my_j + j) % dpt)
            return carry
        lax.fori_loop(1 if i == tiles - 1 else 0, dpt, step, 0, unroll=True)

    def where_is(d):
        return (d // nf, d % nf)

    barrier = pltpu.get_barrier_semaphore()
    for i in range(tiles):
        peers(i, lambda d: pl.semaphore_signal(
            barrier, inc=1, device_id=where_is(d), device_id_type=MESH))

    for copy in small:
        copy.wait()
    q_local = q_ref[...].astype(jnp.float32)
    mine = jnp.concatenate([q_local[:owned], q_local[owned:]], axis=1).astype(jnp.bfloat16)
    q_pack[...] = mine
    my_place = core * chips + me // nf
    q_in[my_place] = mine

    cand_pad[...] = jnp.full(cand_pad.shape, -1, jnp.int32)
    cand_pad[:, :per_query] = cand_ref[...]
    cand = cand_pad[...]
    target = lax.shift_right_arithmetic(cand, jnp.int32(id_bits))
    local = jnp.bitwise_and(cand, jnp.int32(rows_dev - 1))
    low = jnp.bitwise_and(local, jnp.int32(LANES - 1)).astype(jnp.float32)
    high = lax.shift_right_arithmetic(local, jnp.int32(7)).astype(jnp.float32)
    dest = lax.broadcasted_iota(jnp.int32, (n, LANES), 0)
    hot = [jnp.where(target[q:q + 1] == dest, 1.0, 0.0) for q in range(owned)]
    row_i = lax.broadcasted_iota(jnp.int32, (LANES, 2 * LANES), 0)
    col_i = lax.broadcasted_iota(jnp.int32, (LANES, 2 * LANES), 1)
    upper = jnp.where((row_i < col_i) | (col_i >= LANES), 1.0, 0.0).astype(jnp.bfloat16)
    counts = jnp.dot(
        jnp.concatenate(hot, axis=0).astype(jnp.bfloat16), upper, preferred_element_type=jnp.float32)
    base = jnp.zeros((n, LANES), jnp.float32)
    slot = lax.broadcasted_iota(jnp.int32, (LANES, LANES), 0).astype(jnp.float32)
    fields = []
    for q in range(owned):
        block = counts[q * n:(q + 1) * n]
        rank = jnp.sum(hot[q] * (block[:, :LANES] + base), axis=0, keepdims=True)
        base = base + block[:, LANES:]
        places[:, q * LANES:(q + 1) * LANES] = jnp.where(rank == slot, 1.0, 0.0).astype(jnp.bfloat16)
        fields.append(jnp.concatenate(
            [hot[q] * low[q:q + 1], hot[q] * high[q:q + 1], hot[q] * float(q)], axis=0
        ).astype(jnp.bfloat16))
    sorted_fields = lax.dot_general(
        jnp.concatenate(fields, axis=1), places[...], (((1,), (1,)), ((), ())),
        preferred_element_type=jnp.float32)
    packed = (
        sorted_fields[:n] + sorted_fields[n:2 * n] * float(LANES) + sorted_fields[2 * n:] * float(rows_dev)
    ).astype(jnp.int32)
    for t in range(n):
        ids_out[t] = packed[t:t + 1]

    load.wait()

    def widen(b, carry):
        at = pl.ds(pl.multiple_of(b * STEP, STEP), STEP)
        corpus_f[at, :] = corpus_v[at, :].astype(jnp.float32)
        return carry
    lax.fori_loop(0, rows_dev // STEP, widen, 0)

    pl.semaphore_wait(barrier, n - 1)

    def send_queries(d):
        pltpu.make_async_remote_copy(
            src_ref=q_pack, dst_ref=q_in.at[my_place], send_sem=q_send, recv_sem=q_recv.at[my_tile],
            device_id=where_is(d), device_id_type=MESH).start()

    def send_ids(d):
        pltpu.make_async_remote_copy(
            src_ref=ids_out.at[d], dst_ref=ids_in.at[me], send_sem=ids_send, recv_sem=ids_recv,
            device_id=where_is(d), device_id_type=MESH).start()

    peers(0, send_queries)
    for i in range(tiles):
        peers(i, send_ids)
    for i in range(1, tiles - 1):
        for j in range(dpc):
            send_queries((order[i] * dpc + (my_j // nf + j) % dpc) * nf + core)
    peers(tiles - 1, send_queries)
    ids_in[me] = ids_out[me]

    def hand_over(i):
        blocks_of = q_in.at[pl.ds(core * chips + order[i] * dpc, dpc)]
        bulk_wait(q_in.at[pl.ds(0, dpc)], q_recv.at[order[i]])
        pltpu.make_async_remote_copy(
            src_ref=blocks_of, dst_ref=blocks_of, send_sem=hand_send, recv_sem=hand_recv.at[order[i]],
            device_id=where_is(me + 1 - 2 * core), device_id_type=MESH).start()

    def unpack(i):
        if i == 0:
            bulk_wait(q_in.at[pl.ds(0, dpt)], q_recv.at[order[i]])
        elif i == tiles - 1:
            bulk_wait(q_in.at[pl.ds(0, dpt - 1)], q_recv.at[order[i]])
        else:
            bulk_wait(q_in.at[pl.ds(0, dpc)], hand_recv.at[order[i]])
        parts = []
        for g in range(dpc):
            f0 = q_in[order[i] * dpc + g].astype(jnp.float32)
            f1 = q_in[chips + order[i] * dpc + g].astype(jnp.float32)
            parts.append(jnp.where(left, f0, pltpu.roll(f1, half, 1)))
            parts.append(jnp.where(left, pltpu.roll(f0, half, 1), f1))
        asked = jnp.concatenate(parts, axis=0)
        q_full[pl.ds(pl.multiple_of(order[i] * TILE, TILE), TILE), :] = asked.astype(jnp.bfloat16)
        q_turned[order[i]] = asked.T.astype(jnp.bfloat16)

    left = lax.broadcasted_iota(jnp.int32, (owned, LANES), 1) < half
    to_smem = pltpu.make_async_copy(ids_at, ids_sm, sm_sem)
    blocks = rows_dev // BLOCK
    part = n // (2 * blocks)

    def collect(source):
        for r in range(capacity):
            rows_v[source, pl.ds(r, 1), :] = corpus_f[pl.ds(ids_sm[source, 0, r], 1), :]

    def answer(source):
        pairs = lax.dot_general(
            q_full[pl.ds(pl.multiple_of(source * owned, owned), owned), :],
            rows_v[source].astype(jnp.bfloat16),
            (((1,), (1,)), ((), ())), preferred_element_type=jnp.float32)
        who = lax.shift_right_arithmetic(ids_in[source], jnp.int32(id_bits))
        mask = (who == lax.broadcasted_iota(jnp.int32, (owned, LANES), 0)) & (
            lax.broadcasted_iota(jnp.int32, (owned, LANES), 1) < capacity)
        vals_out[source] = jnp.sum(jnp.where(mask, pairs, 0.0), axis=0, keepdims=True)

    gather_first = tiles - 3
    for i in range(tiles):
        tile = order[i]
        if i < tiles - 1:
            unpack(i)
        if i == tiles - 2:
            unpack(tiles - 1)
        cutoff = thr_ref[:, pl.ds(pl.multiple_of(tile * TILE, TILE), TILE)].astype(jnp.float32) * 0.01
        if i == gather_first:
            bulk_wait(ids_in.at[pl.ds(0, n - 1)], ids_recv)
            ids_at[...] = jnp.bitwise_and(ids_in[...], jnp.int32(rows_dev - 1))
            to_smem.start()
            to_smem.wait()

        def sweep(b, acc):
            weights = q_turned[tile]
            sums = []
            for h in range(2):
                at = pl.ds(pl.multiple_of(b * BLOCK + h * (BLOCK // 2), BLOCK // 2), BLOCK // 2)
                scores = jnp.dot(corpus_v[at, :], weights, preferred_element_type=jnp.float32)
                over = jnp.maximum(scores - cutoff, 0.0).reshape(BLOCK // 32, 2, 8, TILE)
                sums.append(jnp.sum(over, axis=0))
            for k in range(part):
                if i == gather_first:
                    collect(b * part + k)
                if i == gather_first + 1:
                    collect(n // 2 + b * part + k)
                    answer(b * part + k)
                    answer(n // 2 + jnp.maximum(b - 1, 0) * part + k)
            return acc[0] + sums[0], acc[1] + sums[1]

        zero = jnp.zeros((2, 8, TILE), jnp.float32)
        acc = lax.fori_loop(0, blocks // 2, sweep, (zero, zero))
        if i + 1 < tiles - 1:
            hand_over(i + 1)
        acc = lax.fori_loop(blocks // 2, blocks, sweep, acc)
        acc = acc[0] + acc[1]
        acc = acc[0] + acc[1]
        total = jnp.sum(acc, axis=0, keepdims=True)
        for h in range(TILE // LANES):
            mass_rows[tile * (TILE // LANES) + h] = total[:, h * LANES:(h + 1) * LANES]

        def send_mass(d):
            pltpu.make_async_remote_copy(
                src_ref=mass_rows.at[d * owned // LANES], dst_ref=mass_in.at[me],
                send_sem=mass_send, recv_sem=mass_recv,
                device_id=where_is(d), device_id_type=MESH).start()
        peers(i, send_mass)
        if i == tiles - 1:
            mass_in[me] = mass_rows[me * owned // LANES]

        if i == gather_first + 1:
            for k in range(part):
                answer(n - part + k)

            def send_vals(d):
                pltpu.make_async_remote_copy(
                    src_ref=vals_out.at[d], dst_ref=vals_in.at[me], send_sem=vals_send, recv_sem=vals_recv,
                    device_id=where_is(d), device_id_type=MESH).start()
            for u in range(tiles):
                peers(u, send_vals)
            vals_in[me] = vals_out[me]

    bulk_wait(vals_in.at[pl.ds(0, n - 1)], vals_recv)
    values = jnp.concatenate([vals_in[t] for t in range(n)], axis=0)
    top = values.astype(jnp.bfloat16)
    rest = values - top.astype(jnp.float32)
    mid = rest.astype(jnp.bfloat16)
    last = (rest - mid.astype(jnp.float32)).astype(jnp.bfloat16)
    pieces = jnp.concatenate([top, mid, last], axis=0)
    cand = cand_pad[...]
    target = lax.shift_right_arithmetic(cand, jnp.int32(id_bits))
    for q in range(owned):
        spread = jnp.dot(
            pieces, places[:, q * LANES:(q + 1) * LANES], preferred_element_type=jnp.float32)
        spread = (spread[2 * n:] + spread[n:2 * n]) + spread[:n]
        ans_out[q:q + 1, :] = jnp.sum(
            jnp.where(target[q:q + 1] == dest, spread, 0.0), axis=0, keepdims=True)

    bulk_wait(mass_in.at[pl.ds(0, n - 1)], mass_recv)
    mass = mass_in[0]
    for t in range(1, n):
        mass = mass + mass_in[t]
    mass = mass * (8.0 / npass_all)
    per_row = LANES // owned
    result = mass
    for u in range(1, per_row):
        result = jnp.where(me % per_row == u, pltpu.roll(mass, LANES - u * owned, 1), result)
    mass_out[...] = result

    bulk_wait(q_in.at[pl.ds(0, 2 * dpt - 1 + (tiles - 2) * dpc)], q_send)
    bulk_wait(q_in.at[pl.ds(0, (tiles - 2) * dpc)], hand_send)
    bulk_wait(ids_in.at[pl.ds(0, n - 1)], ids_send)
    bulk_wait(vals_in.at[pl.ds(0, n - 1)], vals_send)
    bulk_wait(mass_in.at[pl.ds(0, n - 1)], mass_send)


def fused_body(n, nf, queries, corpus, candidates, threshold):
    rows_dev, width = corpus.shape
    owned, per_query = candidates.shape
    nq = n * owned
    capacity = (owned * per_query + n - 1) // n
    vmem = pl.BlockSpec(memory_space=pltpu.VMEM)
    mass, answers = pl.pallas_call(
        functools.partial(kernel, n, nf, rows_dev * n, capacity),
        out_shape=(
            jax.ShapeDtypeStruct((1, LANES), jnp.float32),
            jax.ShapeDtypeStruct((owned, LANES), jnp.float32),
        ),
        in_specs=[pl.BlockSpec(memory_space=pl.ANY)] * 4,
        out_specs=(vmem, vmem),
        scratch_shapes=[
            pltpu.VMEM(queries.shape, jnp.bfloat16),
            pltpu.VMEM((1, nq), jnp.int32),
            pltpu.VMEM((owned, per_query), jnp.int32),
            pltpu.VMEM((rows_dev, width), jnp.bfloat16),
            pltpu.VMEM((rows_dev, width), jnp.float32),
            pltpu.VMEM((owned, LANES), jnp.bfloat16),
            pltpu.VMEM((n, owned, LANES), jnp.bfloat16),
            pltpu.VMEM((nq, LANES), jnp.bfloat16),
            pltpu.VMEM((nq // TILE, LANES, TILE), jnp.bfloat16),
            pltpu.VMEM((owned, LANES), jnp.int32),
            pltpu.VMEM((LANES, owned * LANES), jnp.bfloat16),
            pltpu.VMEM((n, 1, LANES), jnp.int32),
            pltpu.VMEM((n, 1, LANES), jnp.int32),
            pltpu.VMEM((n, 1, LANES), jnp.int32),
            pltpu.SMEM((n, 1, LANES), jnp.int32),
            pltpu.VMEM((n, LANES, LANES), jnp.float32),
            pltpu.VMEM((n, 1, LANES), jnp.float32),
            pltpu.VMEM((n, 1, LANES), jnp.float32),
            pltpu.VMEM((nq // LANES, 1, LANES), jnp.float32),
            pltpu.VMEM((n, 1, LANES), jnp.float32),
            pltpu.SemaphoreType.DMA((3,)),
            pltpu.SemaphoreType.DMA,
            pltpu.SemaphoreType.DMA,
            pltpu.SemaphoreType.DMA,
            pltpu.SemaphoreType.DMA((nq // TILE,)),
            pltpu.SemaphoreType.DMA,
            pltpu.SemaphoreType.DMA((nq // TILE,)),
            pltpu.SemaphoreType.DMA,
            pltpu.SemaphoreType.DMA,
            pltpu.SemaphoreType.DMA,
            pltpu.SemaphoreType.DMA,
            pltpu.SemaphoreType.DMA,
            pltpu.SemaphoreType.DMA,
        ],
        compiler_params=pltpu.CompilerParams(
            collective_id=0, has_side_effects=True),
    )(queries, threshold.reshape(1, nq), candidates, corpus)
    return mass[0, :owned], answers[:, :per_query]


def plain_body(queries, corpus, candidates, threshold):
    rows_dev = corpus.shape[0]
    width = corpus.shape[1]
    shards = lax.axis_size("rows") * lax.axis_size("feat")
    owned_queries = candidates.shape[0]
    per_query = candidates.shape[1]
    npass_all = rows_dev * shards
    cutoff = threshold.astype(jnp.float32) * 0.01
    owner = lax.axis_index(("rows", "feat"))
    full_rows = lax.all_gather(queries, "feat", axis=1, tiled=True)
    whole = lax.all_gather(full_rows, "rows", axis=0, tiled=True)
    query_count = whole.shape[0]
    block = 2048
    corpus_blocks = corpus.reshape(rows_dev // block, block, width)

    def visit(total, block_rows):
        scores = lax.dot_general(
            whole, block_rows, (((1,), (1,)), ((), ())), preferred_element_type=jnp.float32
        )
        return (total + jnp.sum(jnp.maximum(scores - cutoff[:, None], 0.0), axis=1), None)

    total, _ = lax.scan(visit, jnp.zeros((query_count,), jnp.float32), corpus_blocks)
    flat_ids = candidates.reshape(-1)
    total_ids = flat_ids.shape[0]
    capacity = (total_ids + shards - 1) // shards
    target = flat_ids // rows_dev
    onehot = (target[:, None] == jnp.arange(shards, dtype=jnp.int32)[None, :]).astype(jnp.int32)
    before = jnp.cumsum(onehot, axis=0) - onehot
    rank = jnp.sum(before * onehot, axis=1)
    query_ids = owner * owned_queries + jnp.arange(total_ids, dtype=jnp.int32) // per_query
    fields = jnp.stack([flat_ids - target * rows_dev, query_ids], axis=1)
    send_both = jnp.zeros((shards, capacity, 2), jnp.int32).at[target, rank].set(fields)
    n_rows = lax.axis_size("rows")
    n_feat = lax.axis_size("feat")
    received = lax.all_to_all(
        lax.all_to_all(
            send_both.reshape(n_rows, n_feat, capacity * 2),
            "rows",
            split_axis=0,
            concat_axis=0,
            tiled=True,
        ),
        "feat",
        split_axis=1,
        concat_axis=1,
        tiled=True,
    )
    received = received.reshape(shards * capacity, 2)
    picked = corpus[received[:, 0]]
    asked = whole[received[:, 1]]
    values = jnp.einsum("kd,kd->k", picked, asked, preferred_element_type=jnp.float32).reshape(
        n_rows, n_feat, capacity
    )
    partials = total.reshape(n_rows, n_feat, owned_queries)
    answers, mass_parts = (
        lax.all_to_all(
            lax.all_to_all(values, "rows", split_axis=0, concat_axis=0, tiled=True),
            "feat",
            split_axis=1,
            concat_axis=1,
            tiled=True,
        ),
        lax.all_to_all(
            lax.all_to_all(partials, "rows", split_axis=0, concat_axis=0, tiled=True),
            "feat",
            split_axis=1,
            concat_axis=1,
            tiled=True,
        ),
    )
    exceed = jnp.sum(mass_parts, axis=(0, 1)) * (8.0 / npass_all)
    candidate_scores = answers.reshape(shards, capacity)[target, rank].reshape(
        owned_queries, per_query
    )
    return (exceed, candidate_scores)


def body(queries, corpus, candidates, threshold):
    nf = lax.axis_size("feat")
    n = lax.axis_size("rows") * nf
    rows_dev, width = corpus.shape
    owned, per_query = candidates.shape
    capacity = (owned * per_query + n - 1) // n
    fits = (
        nf == 2
        and width == LANES
        and queries.shape == (2 * owned, LANES // 2)
        and owned % 32 == 0
        and LANES % owned == 0
        and per_query <= LANES
        and capacity <= LANES
        and n % 8 == 0
        and (n * owned) % TILE == 0
        and n * owned == 4 * TILE
        and rows_dev % BLOCK == 0
        and n % (2 * (rows_dev // BLOCK)) == 0
        and rows_dev & (rows_dev - 1) == 0
    )
    if fits:
        return fused_body(n, nf, queries, corpus, candidates, threshold)
    return plain_body(queries, corpus, candidates, threshold)


def solution(mesh):
    return jax.shard_map(
        body,
        mesh=mesh,
        in_specs=(P("rows", "feat"), P(("rows", "feat"), None), P(("rows", "feat"), None), P()),
        out_specs=(P(("rows", "feat")), P(("rows", "feat"), None)),
        check_vma=False,
    )
```

```python
import functools

import jax
import jax.numpy as jnp
from jax import lax
from jax.experimental import pallas as pl
from jax.experimental.pallas import tpu as pltpu
from jax.sharding import PartitionSpec as P

LANES = 128
TILE = 256
BLOCK = 4096
STEP = 512
MESH = pl.DeviceIdType.MESH


def bulk_wait(ref, sem):
    pltpu.make_async_copy(ref, ref, sem).wait()


def kernel(
    n, nf, npass_all, capacity,
    q_hbm, thr_hbm, cand_hbm, corpus_ref,
    mass_out, ans_out,
    q_ref, thr_ref, cand_ref, corpus_v, corpus_f, q_pack, q_in, q_full, q_turned, cand_pad, places,
    ids_out, ids_in, ids_at, ids_sm, rows_v, vals_out, vals_in, mass_rows, mass_in,
    small_sem, load_sem, sm_sem, q_send, q_recv, hand_send, hand_recv, far_sem, ids_send, ids_recv, vals_send, vals_recv, mass_send, mass_recv,
):
    rows_dev, width = corpus_v.shape
    owned, per_query = cand_ref.shape
    nq = q_full.shape[0]
    half = q_ref.shape[1]
    tiles = nq // TILE
    dpt = TILE // owned
    chips = n // nf
    dpc = dpt // nf
    core = lax.axis_index("feat")
    me = lax.axis_index("rows") * nf + core
    my_tile = me // dpt
    my_j = me % dpt
    id_bits = rows_dev.bit_length() - 1
    beside = my_tile + 1 - 2 * (my_tile % 2)
    order = [beside]
    for k in range(1, tiles // 2):
        order += [(my_tile + 2 * k) % tiles, (beside + 2 * k) % tiles]
    order.append(my_tile)

    load = pltpu.make_async_copy(corpus_ref, corpus_v, load_sem)
    small = [
        pltpu.make_async_copy(src, dst, small_sem.at[k])
        for k, (src, dst) in enumerate(((q_hbm, q_ref), (cand_hbm, cand_ref), (thr_hbm, thr_ref)))]
    for copy in small:
        copy.start()
    load.start()

    def peers(i, act):
        def step(j, carry):
            act(order[i] * dpt + (my_j + j) % dpt)
            return carry
        lax.fori_loop(1 if i == tiles - 1 else 0, dpt, step, 0, unroll=True)

    def where_is(d):
        return (d // nf, d % nf)

    barrier = pltpu.get_barrier_semaphore()
    inner = (my_tile >= 1) & (my_tile < tiles - 1)
    across = (tiles - 1 - my_tile) * dpt + my_j
    nearby = beside * dpt + my_j

    def signal(sem, d):
        pl.semaphore_signal(sem, inc=1, device_id=where_is(d), device_id_type=MESH)

    @pl.when(inner)
    def _():
        signal(barrier, across)
    peers(0, functools.partial(signal, barrier))
    peers(tiles - 1, functools.partial(signal, barrier))

    for copy in small:
        copy.wait()
    q_local = q_ref[...].astype(jnp.float32)
    mine = jnp.concatenate([q_local[:owned], q_local[owned:]], axis=1).astype(jnp.bfloat16)
    q_pack[...] = mine
    my_place = core * chips + me // nf
    q_in[my_place] = mine

    cand_pad[...] = jnp.full(cand_pad.shape, -1, jnp.int32)
    cand_pad[:, :per_query] = cand_ref[...]
    cand = cand_pad[...]
    target = lax.shift_right_arithmetic(cand, jnp.int32(id_bits))
    local = jnp.bitwise_and(cand, jnp.int32(rows_dev - 1))
    low = jnp.bitwise_and(local, jnp.int32(LANES - 1)).astype(jnp.float32)
    high = lax.shift_right_arithmetic(local, jnp.int32(7)).astype(jnp.float32)
    dest = lax.broadcasted_iota(jnp.int32, (n, LANES), 0)
    hot = [jnp.where(target[q:q + 1] == dest, 1.0, 0.0) for q in range(owned)]
    row_i = lax.broadcasted_iota(jnp.int32, (LANES, 2 * LANES), 0)
    col_i = lax.broadcasted_iota(jnp.int32, (LANES, 2 * LANES), 1)
    upper = jnp.where((row_i < col_i) | (col_i >= LANES), 1.0, 0.0).astype(jnp.bfloat16)
    counts = jnp.dot(
        jnp.concatenate(hot, axis=0).astype(jnp.bfloat16), upper, preferred_element_type=jnp.float32)
    base = jnp.zeros((n, LANES), jnp.float32)
    slot = lax.broadcasted_iota(jnp.int32, (LANES, LANES), 0).astype(jnp.float32)
    fields = []
    for q in range(owned):
        block = counts[q * n:(q + 1) * n]
        rank = jnp.sum(hot[q] * (block[:, :LANES] + base), axis=0, keepdims=True)
        base = base + block[:, LANES:]
        places[:, q * LANES:(q + 1) * LANES] = jnp.where(rank == slot, 1.0, 0.0).astype(jnp.bfloat16)
        fields.append(jnp.concatenate(
            [hot[q] * low[q:q + 1], hot[q] * high[q:q + 1], hot[q] * float(q)], axis=0
        ).astype(jnp.bfloat16))
    sorted_fields = lax.dot_general(
        jnp.concatenate(fields, axis=1), places[...], (((1,), (1,)), ((), ())),
        preferred_element_type=jnp.float32)
    packed = (
        sorted_fields[:n] + sorted_fields[n:2 * n] * float(LANES) + sorted_fields[2 * n:] * float(rows_dev)
    ).astype(jnp.int32)
    for t in range(n):
        ids_out[t] = packed[t:t + 1]

    load.wait()

    def widen(b, carry):
        at = pl.ds(pl.multiple_of(b * STEP, STEP), STEP)
        corpus_f[at, :] = corpus_v[at, :].astype(jnp.float32)
        return carry
    lax.fori_loop(0, rows_dev // STEP, widen, 0)

    @pl.when(inner)
    def _():
        pl.semaphore_wait(barrier, 2 * dpt)

    @pl.when(jnp.logical_not(inner))
    def _():
        pl.semaphore_wait(barrier, 2 * dpt - 1)

    def send_queries(d):
        pltpu.make_async_remote_copy(
            src_ref=q_pack, dst_ref=q_in.at[my_place], send_sem=q_send, recv_sem=q_recv.at[my_tile],
            device_id=where_is(d), device_id_type=MESH).start()

    def send_ids(d):
        pltpu.make_async_remote_copy(
            src_ref=ids_out.at[d], dst_ref=ids_in.at[me], send_sem=ids_send, recv_sem=ids_recv,
            device_id=where_is(d), device_id_type=MESH).start()

    @pl.when(inner)
    def _():
        signal(far_sem, across)
    peers(0, send_queries)
    peers(0, send_ids)
    peers(tiles - 1, send_ids)
    pl.semaphore_wait(far_sem, 1)

    @pl.when(inner)
    def _():
        signal(far_sem, nearby)
    for i in range(1, tiles - 1):
        peers(i, send_ids)
    for i in range(1, tiles - 1):
        for j in range(dpc):
            send_queries((order[i] * dpc + (my_j // nf + j) % dpc) * nf + core)
    peers(tiles - 1, send_queries)
    ids_in[me] = ids_out[me]

    def hand_over(i):
        blocks_of = q_in.at[pl.ds(core * chips + order[i] * dpc, dpc)]
        bulk_wait(q_in.at[pl.ds(0, dpc)], q_recv.at[order[i]])
        pltpu.make_async_remote_copy(
            src_ref=blocks_of, dst_ref=blocks_of, send_sem=hand_send, recv_sem=hand_recv.at[order[i]],
            device_id=where_is(me + 1 - 2 * core), device_id_type=MESH).start()

    def unpack(i):
        if i == 0:
            bulk_wait(q_in.at[pl.ds(0, dpt)], q_recv.at[order[i]])
        elif i == tiles - 1:
            bulk_wait(q_in.at[pl.ds(0, dpt - 1)], q_recv.at[order[i]])
        else:
            bulk_wait(q_in.at[pl.ds(0, dpc)], hand_recv.at[order[i]])
        parts = []
        for g in range(dpc):
            f0 = q_in[order[i] * dpc + g].astype(jnp.float32)
            f1 = q_in[chips + order[i] * dpc + g].astype(jnp.float32)
            parts.append(jnp.where(left, f0, pltpu.roll(f1, half, 1)))
            parts.append(jnp.where(left, pltpu.roll(f0, half, 1), f1))
        asked = jnp.concatenate(parts, axis=0)
        q_full[pl.ds(pl.multiple_of(order[i] * TILE, TILE), TILE), :] = asked.astype(jnp.bfloat16)
        q_turned[order[i]] = asked.T.astype(jnp.bfloat16)

    left = lax.broadcasted_iota(jnp.int32, (owned, LANES), 1) < half
    to_smem = pltpu.make_async_copy(ids_at, ids_sm, sm_sem)
    blocks = rows_dev // BLOCK
    part = n // (2 * blocks)

    def collect(source):
        for r in range(capacity):
            rows_v[source, pl.ds(r, 1), :] = corpus_f[pl.ds(ids_sm[source, 0, r], 1), :]

    def answer(source):
        pairs = lax.dot_general(
            q_full[pl.ds(pl.multiple_of(source * owned, owned), owned), :],
            rows_v[source].astype(jnp.bfloat16),
            (((1,), (1,)), ((), ())), preferred_element_type=jnp.float32)
        who = lax.shift_right_arithmetic(ids_in[source], jnp.int32(id_bits))
        mask = (who == lax.broadcasted_iota(jnp.int32, (owned, LANES), 0)) & (
            lax.broadcasted_iota(jnp.int32, (owned, LANES), 1) < capacity)
        vals_out[source] = jnp.sum(jnp.where(mask, pairs, 0.0), axis=0, keepdims=True)

    gather_first = tiles - 3
    for i in range(tiles):
        tile = order[i]
        if i < tiles - 1:
            unpack(i)
        if i == tiles - 2:
            unpack(tiles - 1)
        cutoff = thr_ref[:, pl.ds(pl.multiple_of(tile * TILE, TILE), TILE)].astype(jnp.float32) * 0.01
        if i == gather_first:
            bulk_wait(ids_in.at[pl.ds(0, n - 1)], ids_recv)
            ids_at[...] = jnp.bitwise_and(ids_in[...], jnp.int32(rows_dev - 1))
            to_smem.start()
            to_smem.wait()

        def sweep(b, acc):
            weights = q_turned[tile]
            sums = []
            for h in range(2):
                at = pl.ds(pl.multiple_of(b * BLOCK + h * (BLOCK // 2), BLOCK // 2), BLOCK // 2)
                scores = jnp.dot(corpus_v[at, :], weights, preferred_element_type=jnp.float32)
                over = jnp.maximum(scores - cutoff, 0.0).reshape(BLOCK // 32, 2, 8, TILE)
                sums.append(jnp.sum(over, axis=0))
            for k in range(part):
                if i == gather_first:
                    collect(b * part + k)
                if i == gather_first + 1:
                    collect(n // 2 + b * part + k)
                    answer(b * part + k)
                    answer(n // 2 + jnp.maximum(b - 1, 0) * part + k)
            return acc[0] + sums[0], acc[1] + sums[1]

        zero = jnp.zeros((2, 8, TILE), jnp.float32)
        acc = lax.fori_loop(0, blocks // 2, sweep, (zero, zero))
        if i + 1 < tiles - 1:
            hand_over(i + 1)
        acc = lax.fori_loop(blocks // 2, blocks, sweep, acc)
        acc = acc[0] + acc[1]
        acc = acc[0] + acc[1]
        total = jnp.sum(acc, axis=0, keepdims=True)
        for h in range(TILE // LANES):
            mass_rows[tile * (TILE // LANES) + h] = total[:, h * LANES:(h + 1) * LANES]

        def send_mass(d):
            pltpu.make_async_remote_copy(
                src_ref=mass_rows.at[d * owned // LANES], dst_ref=mass_in.at[me],
                send_sem=mass_send, recv_sem=mass_recv,
                device_id=where_is(d), device_id_type=MESH).start()
        peers(i, send_mass)
        if i == tiles - 1:
            mass_in[me] = mass_rows[me * owned // LANES]

        if i == gather_first + 1:
            for k in range(part):
                answer(n - part + k)

            def send_vals(d):
                pltpu.make_async_remote_copy(
                    src_ref=vals_out.at[d], dst_ref=vals_in.at[me], send_sem=vals_send, recv_sem=vals_recv,
                    device_id=where_is(d), device_id_type=MESH).start()
            for u in range(tiles):
                peers(u, send_vals)
            vals_in[me] = vals_out[me]

    bulk_wait(vals_in.at[pl.ds(0, n - 1)], vals_recv)
    values = jnp.concatenate([vals_in[t] for t in range(n)], axis=0)
    top = values.astype(jnp.bfloat16)
    rest = values - top.astype(jnp.float32)
    mid = rest.astype(jnp.bfloat16)
    last = (rest - mid.astype(jnp.float32)).astype(jnp.bfloat16)
    pieces = jnp.concatenate([top, mid, last], axis=0)
    cand = cand_pad[...]
    target = lax.shift_right_arithmetic(cand, jnp.int32(id_bits))
    for q in range(owned):
        spread = jnp.dot(
            pieces, places[:, q * LANES:(q + 1) * LANES], preferred_element_type=jnp.float32)
        spread = (spread[2 * n:] + spread[n:2 * n]) + spread[:n]
        ans_out[q:q + 1, :] = jnp.sum(
            jnp.where(target[q:q + 1] == dest, spread, 0.0), axis=0, keepdims=True)

    bulk_wait(mass_in.at[pl.ds(0, n - 1)], mass_recv)
    mass = mass_in[0]
    for t in range(1, n):
        mass = mass + mass_in[t]
    mass = mass * (8.0 / npass_all)
    per_row = LANES // owned
    result = mass
    for u in range(1, per_row):
        result = jnp.where(me % per_row == u, pltpu.roll(mass, LANES - u * owned, 1), result)
    mass_out[...] = result

    bulk_wait(q_in.at[pl.ds(0, 2 * dpt - 1 + (tiles - 2) * dpc)], q_send)
    bulk_wait(q_in.at[pl.ds(0, (tiles - 2) * dpc)], hand_send)
    bulk_wait(ids_in.at[pl.ds(0, n - 1)], ids_send)
    bulk_wait(vals_in.at[pl.ds(0, n - 1)], vals_send)
    bulk_wait(mass_in.at[pl.ds(0, n - 1)], mass_send)


def fused_body(n, nf, queries, corpus, candidates, threshold):
    rows_dev, width = corpus.shape
    owned, per_query = candidates.shape
    nq = n * owned
    capacity = (owned * per_query + n - 1) // n
    vmem = pl.BlockSpec(memory_space=pltpu.VMEM)
    mass, answers = pl.pallas_call(
        functools.partial(kernel, n, nf, rows_dev * n, capacity),
        out_shape=(
            jax.ShapeDtypeStruct((1, LANES), jnp.float32),
            jax.ShapeDtypeStruct((owned, LANES), jnp.float32),
        ),
        in_specs=[pl.BlockSpec(memory_space=pl.ANY)] * 4,
        out_specs=(vmem, vmem),
        scratch_shapes=[
            pltpu.VMEM(queries.shape, jnp.bfloat16),
            pltpu.VMEM((1, nq), jnp.int32),
            pltpu.VMEM((owned, per_query), jnp.int32),
            pltpu.VMEM((rows_dev, width), jnp.bfloat16),
            pltpu.VMEM((rows_dev, width), jnp.float32),
            pltpu.VMEM((owned, LANES), jnp.bfloat16),
            pltpu.VMEM((n, owned, LANES), jnp.bfloat16),
            pltpu.VMEM((nq, LANES), jnp.bfloat16),
            pltpu.VMEM((nq // TILE, LANES, TILE), jnp.bfloat16),
            pltpu.VMEM((owned, LANES), jnp.int32),
            pltpu.VMEM((LANES, owned * LANES), jnp.bfloat16),
            pltpu.VMEM((n, 1, LANES), jnp.int32),
            pltpu.VMEM((n, 1, LANES), jnp.int32),
            pltpu.VMEM((n, 1, LANES), jnp.int32),
            pltpu.SMEM((n, 1, LANES), jnp.int32),
            pltpu.VMEM((n, LANES, LANES), jnp.float32),
            pltpu.VMEM((n, 1, LANES), jnp.float32),
            pltpu.VMEM((n, 1, LANES), jnp.float32),
            pltpu.VMEM((nq // LANES, 1, LANES), jnp.float32),
            pltpu.VMEM((n, 1, LANES), jnp.float32),
            pltpu.SemaphoreType.DMA((3,)),
            pltpu.SemaphoreType.DMA,
            pltpu.SemaphoreType.DMA,
            pltpu.SemaphoreType.DMA,
            pltpu.SemaphoreType.DMA((nq // TILE,)),
            pltpu.SemaphoreType.DMA,
            pltpu.SemaphoreType.DMA((nq // TILE,)),
            pltpu.SemaphoreType.REGULAR,
            pltpu.SemaphoreType.DMA,
            pltpu.SemaphoreType.DMA,
            pltpu.SemaphoreType.DMA,
            pltpu.SemaphoreType.DMA,
            pltpu.SemaphoreType.DMA,
            pltpu.SemaphoreType.DMA,
        ],
        compiler_params=pltpu.CompilerParams(
            collective_id=0, has_side_effects=True),
    )(queries, threshold.reshape(1, nq), candidates, corpus)
    return mass[0, :owned], answers[:, :per_query]


def plain_body(queries, corpus, candidates, threshold):
    rows_dev = corpus.shape[0]
    width = corpus.shape[1]
    shards = lax.axis_size("rows") * lax.axis_size("feat")
    owned_queries = candidates.shape[0]
    per_query = candidates.shape[1]
    npass_all = rows_dev * shards
    cutoff = threshold.astype(jnp.float32) * 0.01
    owner = lax.axis_index(("rows", "feat"))
    full_rows = lax.all_gather(queries, "feat", axis=1, tiled=True)
    whole = lax.all_gather(full_rows, "rows", axis=0, tiled=True)
    query_count = whole.shape[0]
    block = 2048
    corpus_blocks = corpus.reshape(rows_dev // block, block, width)

    def visit(total, block_rows):
        scores = lax.dot_general(
            whole, block_rows, (((1,), (1,)), ((), ())), preferred_element_type=jnp.float32
        )
        return (total + jnp.sum(jnp.maximum(scores - cutoff[:, None], 0.0), axis=1), None)

    total, _ = lax.scan(visit, jnp.zeros((query_count,), jnp.float32), corpus_blocks)
    flat_ids = candidates.reshape(-1)
    total_ids = flat_ids.shape[0]
    capacity = (total_ids + shards - 1) // shards
    target = flat_ids // rows_dev
    onehot = (target[:, None] == jnp.arange(shards, dtype=jnp.int32)[None, :]).astype(jnp.int32)
    before = jnp.cumsum(onehot, axis=0) - onehot
    rank = jnp.sum(before * onehot, axis=1)
    query_ids = owner * owned_queries + jnp.arange(total_ids, dtype=jnp.int32) // per_query
    fields = jnp.stack([flat_ids - target * rows_dev, query_ids], axis=1)
    send_both = jnp.zeros((shards, capacity, 2), jnp.int32).at[target, rank].set(fields)
    n_rows = lax.axis_size("rows")
    n_feat = lax.axis_size("feat")
    received = lax.all_to_all(
        lax.all_to_all(
            send_both.reshape(n_rows, n_feat, capacity * 2),
            "rows",
            split_axis=0,
            concat_axis=0,
            tiled=True,
        ),
        "feat",
        split_axis=1,
        concat_axis=1,
        tiled=True,
    )
    received = received.reshape(shards * capacity, 2)
    picked = corpus[received[:, 0]]
    asked = whole[received[:, 1]]
    values = jnp.einsum("kd,kd->k", picked, asked, preferred_element_type=jnp.float32).reshape(
        n_rows, n_feat, capacity
    )
    partials = total.reshape(n_rows, n_feat, owned_queries)
    answers, mass_parts = (
        lax.all_to_all(
            lax.all_to_all(values, "rows", split_axis=0, concat_axis=0, tiled=True),
            "feat",
            split_axis=1,
            concat_axis=1,
            tiled=True,
        ),
        lax.all_to_all(
            lax.all_to_all(partials, "rows", split_axis=0, concat_axis=0, tiled=True),
            "feat",
            split_axis=1,
            concat_axis=1,
            tiled=True,
        ),
    )
    exceed = jnp.sum(mass_parts, axis=(0, 1)) * (8.0 / npass_all)
    candidate_scores = answers.reshape(shards, capacity)[target, rank].reshape(
        owned_queries, per_query
    )
    return (exceed, candidate_scores)


def body(queries, corpus, candidates, threshold):
    nf = lax.axis_size("feat")
    n = lax.axis_size("rows") * nf
    rows_dev, width = corpus.shape
    owned, per_query = candidates.shape
    capacity = (owned * per_query + n - 1) // n
    fits = (
        nf == 2
        and width == LANES
        and queries.shape == (2 * owned, LANES // 2)
        and owned % 32 == 0
        and LANES % owned == 0
        and per_query <= LANES
        and capacity <= LANES
        and n % 8 == 0
        and (n * owned) % TILE == 0
        and n * owned == 4 * TILE
        and rows_dev % BLOCK == 0
        and n % (2 * (rows_dev // BLOCK)) == 0
        and rows_dev & (rows_dev - 1) == 0
    )
    if fits:
        return fused_body(n, nf, queries, corpus, candidates, threshold)
    return plain_body(queries, corpus, candidates, threshold)


def solution(mesh):
    return jax.shard_map(
        body,
        mesh=mesh,
        in_specs=(P("rows", "feat"), P(("rows", "feat"), None), P(("rows", "feat"), None), P()),
        out_specs=(P(("rows", "feat")), P(("rows", "feat"), None)),
        check_vma=False,
    )
```

```python
import functools

import jax
import jax.numpy as jnp
from jax import lax
from jax.experimental import pallas as pl
from jax.experimental.pallas import tpu as pltpu
from jax.sharding import PartitionSpec as P

LANES = 128
TILE = 256
BLOCK = 4096
MIXED = 2048
STEP = 512
MESH = pl.DeviceIdType.MESH


def bulk_wait(ref, sem):
    pltpu.make_async_copy(ref, ref, sem).wait()


def kernel(
    n, nf, npass_all, capacity,
    q_hbm, thr_hbm, cand_hbm, corpus_ref,
    mass_out, ans_out,
    q_ref, thr_ref, cand_ref, corpus_v, corpus_f, q_pack, q_in, q_full, q_turned, cand_pad, places,
    ids_out, ids_in, ids_at, ids_sm, rows_v, vals_out, vals_in, mass_rows, mass_in,
    small_sem, load_sem, sm_sem, q_send, q_recv, hand_send, hand_recv, far_sem, ids_send, ids_recv, vals_send, vals_recv, mass_send, mass_recv,
):
    rows_dev, width = corpus_v.shape
    owned, per_query = cand_ref.shape
    nq = q_full.shape[0]
    half = q_ref.shape[1]
    tiles = nq // TILE
    dpt = TILE // owned
    chips = n // nf
    dpc = dpt // nf
    core = lax.axis_index("feat")
    me = lax.axis_index("rows") * nf + core
    my_tile = me // dpt
    my_j = me % dpt
    id_bits = rows_dev.bit_length() - 1
    beside = my_tile + 1 - 2 * (my_tile % 2)
    order = [beside]
    for k in range(1, tiles // 2):
        order += [(my_tile + 2 * k) % tiles, (beside + 2 * k) % tiles]
    order.append(my_tile)

    load = pltpu.make_async_copy(corpus_ref, corpus_v, load_sem)
    small = [
        pltpu.make_async_copy(src, dst, small_sem.at[k])
        for k, (src, dst) in enumerate(((q_hbm, q_ref), (cand_hbm, cand_ref), (thr_hbm, thr_ref)))]
    for copy in small:
        copy.start()
    load.start()

    def peers(i, act):
        def step(j, carry):
            act(order[i] * dpt + (my_j + j) % dpt)
            return carry
        lax.fori_loop(1 if i == tiles - 1 else 0, dpt, step, 0, unroll=True)

    def where_is(d):
        return (d // nf, d % nf)

    barrier = pltpu.get_barrier_semaphore()
    inner = (my_tile >= 1) & (my_tile < tiles - 1)
    across = (tiles - 1 - my_tile) * dpt + my_j
    nearby = beside * dpt + my_j

    def signal(sem, d):
        pl.semaphore_signal(sem, inc=1, device_id=where_is(d), device_id_type=MESH)

    @pl.when(inner)
    def _():
        signal(barrier, across)
    peers(0, functools.partial(signal, barrier))
    peers(tiles - 1, functools.partial(signal, barrier))

    for copy in small:
        copy.wait()
    q_local = q_ref[...].astype(jnp.float32)
    mine = jnp.concatenate([q_local[:owned], q_local[owned:]], axis=1).astype(jnp.bfloat16)
    q_pack[...] = mine
    my_place = core * chips + me // nf
    q_in[my_place] = mine

    cand_pad[...] = jnp.full(cand_pad.shape, -1, jnp.int32)
    cand_pad[:, :per_query] = cand_ref[...]
    cand = cand_pad[...]
    target = lax.shift_right_arithmetic(cand, jnp.int32(id_bits))
    local = jnp.bitwise_and(cand, jnp.int32(rows_dev - 1))
    low = jnp.bitwise_and(local, jnp.int32(LANES - 1)).astype(jnp.float32)
    high = lax.shift_right_arithmetic(local, jnp.int32(7)).astype(jnp.float32)
    dest = lax.broadcasted_iota(jnp.int32, (n, LANES), 0)
    hot = [jnp.where(target[q:q + 1] == dest, 1.0, 0.0) for q in range(owned)]
    row_i = lax.broadcasted_iota(jnp.int32, (LANES, 2 * LANES), 0)
    col_i = lax.broadcasted_iota(jnp.int32, (LANES, 2 * LANES), 1)
    upper = jnp.where((row_i < col_i) | (col_i >= LANES), 1.0, 0.0).astype(jnp.bfloat16)
    counts = jnp.dot(
        jnp.concatenate(hot, axis=0).astype(jnp.bfloat16), upper, preferred_element_type=jnp.float32)
    base = jnp.zeros((n, LANES), jnp.float32)
    slot = lax.broadcasted_iota(jnp.int32, (LANES, LANES), 0).astype(jnp.float32)
    fields = []
    for q in range(owned):
        block = counts[q * n:(q + 1) * n]
        rank = jnp.sum(hot[q] * (block[:, :LANES] + base), axis=0, keepdims=True)
        base = base + block[:, LANES:]
        places[:, q * LANES:(q + 1) * LANES] = jnp.where(rank == slot, 1.0, 0.0).astype(jnp.bfloat16)
        fields.append(jnp.concatenate(
            [hot[q] * low[q:q + 1], hot[q] * high[q:q + 1], hot[q] * float(q)], axis=0
        ).astype(jnp.bfloat16))
    sorted_fields = lax.dot_general(
        jnp.concatenate(fields, axis=1), places[...], (((1,), (1,)), ((), ())),
        preferred_element_type=jnp.float32)
    packed = (
        sorted_fields[:n] + sorted_fields[n:2 * n] * float(LANES) + sorted_fields[2 * n:] * float(rows_dev)
    ).astype(jnp.int32)
    for t in range(n):
        ids_out[t] = packed[t:t + 1]

    load.wait()

    def widen(b, carry):
        at = pl.ds(pl.multiple_of(b * STEP, STEP), STEP)
        corpus_f[at, :] = corpus_v[at, :].astype(jnp.float32)
        return carry
    lax.fori_loop(0, rows_dev // STEP, widen, 0)

    @pl.when(inner)
    def _():
        pl.semaphore_wait(barrier, 2 * dpt)

    @pl.when(jnp.logical_not(inner))
    def _():
        pl.semaphore_wait(barrier, 2 * dpt - 1)

    def send_queries(d):
        pltpu.make_async_remote_copy(
            src_ref=q_pack, dst_ref=q_in.at[my_place], send_sem=q_send, recv_sem=q_recv.at[my_tile],
            device_id=where_is(d), device_id_type=MESH).start()

    def send_ids(d):
        pltpu.make_async_remote_copy(
            src_ref=ids_out.at[d], dst_ref=ids_in.at[me], send_sem=ids_send, recv_sem=ids_recv,
            device_id=where_is(d), device_id_type=MESH).start()

    @pl.when(inner)
    def _():
        signal(far_sem, across)
    peers(0, send_queries)
    peers(tiles - 1, send_queries)
    peers(0, send_ids)
    peers(tiles - 1, send_ids)
    pl.semaphore_wait(far_sem, 1)

    @pl.when(inner)
    def _():
        signal(far_sem, nearby)
    for i in range(1, tiles - 1):
        peers(i, send_ids)
    for i in range(1, tiles - 1):
        for j in range(dpc):
            send_queries((order[i] * dpc + (my_j // nf + j) % dpc) * nf + core)
    ids_in[me] = ids_out[me]

    def hand_over(i):
        blocks_of = q_in.at[pl.ds(core * chips + order[i] * dpc, dpc)]
        bulk_wait(q_in.at[pl.ds(0, dpc)], q_recv.at[order[i]])
        pltpu.make_async_remote_copy(
            src_ref=blocks_of, dst_ref=blocks_of, send_sem=hand_send, recv_sem=hand_recv.at[order[i]],
            device_id=where_is(me + 1 - 2 * core), device_id_type=MESH).start()

    def unpack(i):
        if i == 0:
            bulk_wait(q_in.at[pl.ds(0, dpt)], q_recv.at[order[i]])
        elif i == tiles - 1:
            bulk_wait(q_in.at[pl.ds(0, dpt - 1)], q_recv.at[order[i]])
        else:
            bulk_wait(q_in.at[pl.ds(0, dpc)], hand_recv.at[order[i]])
        parts = []
        for g in range(dpc):
            f0 = q_in[order[i] * dpc + g].astype(jnp.float32)
            f1 = q_in[chips + order[i] * dpc + g].astype(jnp.float32)
            parts.append(jnp.where(left, f0, pltpu.roll(f1, half, 1)))
            parts.append(jnp.where(left, pltpu.roll(f0, half, 1), f1))
        asked = jnp.concatenate(parts, axis=0)
        q_full[pl.ds(pl.multiple_of(order[i] * TILE, TILE), TILE), :] = asked.astype(jnp.bfloat16)
        q_turned[order[i]] = asked.T.astype(jnp.bfloat16)

    left = lax.broadcasted_iota(jnp.int32, (owned, LANES), 1) < half
    to_smem = pltpu.make_async_copy(ids_at, ids_sm, sm_sem)
    gather_tile = tiles - 2
    part = n // (rows_dev // MIXED)

    def collect(source):
        for r in range(capacity):
            rows_v[source, pl.ds(r, 1), :] = corpus_f[pl.ds(ids_sm[source, 0, r], 1), :]

    def answer(source):
        pairs = lax.dot_general(
            q_full[pl.ds(pl.multiple_of(source * owned, owned), owned), :],
            rows_v[source].astype(jnp.bfloat16),
            (((1,), (1,)), ((), ())), preferred_element_type=jnp.float32)
        who = lax.shift_right_arithmetic(ids_in[source], jnp.int32(id_bits))
        mask = (who == lax.broadcasted_iota(jnp.int32, (owned, LANES), 0)) & (
            lax.broadcasted_iota(jnp.int32, (owned, LANES), 1) < capacity)
        vals_out[source] = jnp.sum(jnp.where(mask, pairs, 0.0), axis=0, keepdims=True)

    unpack(tiles - 1)
    for i in range(tiles):
        tile = order[i]
        if i < tiles - 1:
            unpack(i)
        size = MIXED if i == gather_tile else BLOCK
        blocks = rows_dev // size
        cutoff = thr_ref[:, pl.ds(pl.multiple_of(tile * TILE, TILE), TILE)].astype(jnp.float32) * 0.01
        if i == gather_tile:
            to_smem.wait()

        def sweep(b, acc):
            weights = q_turned[tile]
            sums = []
            for h in range(2):
                at = pl.ds(pl.multiple_of(b * size + h * (size // 2), size // 2), size // 2)
                scores = jnp.dot(corpus_v[at, :], weights, preferred_element_type=jnp.float32)
                over = jnp.maximum(scores - cutoff, 0.0).reshape(size // 32, 2, 8, TILE)
                sums.append(jnp.sum(over, axis=0))
            if i == gather_tile:
                for k in range(part):
                    collect(b * part + k)
                    answer(jnp.maximum(b - 1, 0) * part + k)
            return acc[0] + sums[0], acc[1] + sums[1]

        zero = jnp.zeros((2, 8, TILE), jnp.float32)
        acc = lax.fori_loop(0, blocks // 2, sweep, (zero, zero))
        if i + 1 < tiles - 1:
            hand_over(i + 1)
        if i == gather_tile - 1:
            bulk_wait(ids_in.at[pl.ds(0, n - 1)], ids_recv)
            ids_at[...] = jnp.bitwise_and(ids_in[...], jnp.int32(rows_dev - 1))
            to_smem.start()
        acc = lax.fori_loop(blocks // 2, blocks, sweep, acc)
        acc = acc[0] + acc[1]
        acc = acc[0] + acc[1]
        total = jnp.sum(acc, axis=0, keepdims=True)
        for h in range(TILE // LANES):
            mass_rows[tile * (TILE // LANES) + h] = total[:, h * LANES:(h + 1) * LANES]

        def send_mass(d):
            pltpu.make_async_remote_copy(
                src_ref=mass_rows.at[d * owned // LANES], dst_ref=mass_in.at[me],
                send_sem=mass_send, recv_sem=mass_recv,
                device_id=where_is(d), device_id_type=MESH).start()
        peers(i, send_mass)
        if i == tiles - 1:
            mass_in[me] = mass_rows[me * owned // LANES]

        if i == gather_tile:
            for k in range(part):
                answer(n - part + k)

            def send_vals(d):
                pltpu.make_async_remote_copy(
                    src_ref=vals_out.at[d], dst_ref=vals_in.at[me], send_sem=vals_send, recv_sem=vals_recv,
                    device_id=where_is(d), device_id_type=MESH).start()
            for u in range(tiles):
                peers(u, send_vals)
            vals_in[me] = vals_out[me]

    bulk_wait(vals_in.at[pl.ds(0, n - 1)], vals_recv)
    values = jnp.concatenate([vals_in[t] for t in range(n)], axis=0)
    top = values.astype(jnp.bfloat16)
    rest = values - top.astype(jnp.float32)
    mid = rest.astype(jnp.bfloat16)
    last = (rest - mid.astype(jnp.float32)).astype(jnp.bfloat16)
    pieces = jnp.concatenate([top, mid, last], axis=0)
    cand = cand_pad[...]
    target = lax.shift_right_arithmetic(cand, jnp.int32(id_bits))
    for q in range(owned):
        spread = jnp.dot(
            pieces, places[:, q * LANES:(q + 1) * LANES], preferred_element_type=jnp.float32)
        spread = (spread[2 * n:] + spread[n:2 * n]) + spread[:n]
        ans_out[q:q + 1, :] = jnp.sum(
            jnp.where(target[q:q + 1] == dest, spread, 0.0), axis=0, keepdims=True)

    bulk_wait(mass_in.at[pl.ds(0, n - 1)], mass_recv)
    mass = mass_in[0]
    for t in range(1, n):
        mass = mass + mass_in[t]
    mass = mass * (8.0 / npass_all)
    per_row = LANES // owned
    result = mass
    for u in range(1, per_row):
        result = jnp.where(me % per_row == u, pltpu.roll(mass, LANES - u * owned, 1), result)
    mass_out[...] = result

    bulk_wait(q_in.at[pl.ds(0, 2 * dpt - 1 + (tiles - 2) * dpc)], q_send)
    bulk_wait(q_in.at[pl.ds(0, (tiles - 2) * dpc)], hand_send)
    bulk_wait(ids_in.at[pl.ds(0, n - 1)], ids_send)
    bulk_wait(vals_in.at[pl.ds(0, n - 1)], vals_send)
    bulk_wait(mass_in.at[pl.ds(0, n - 1)], mass_send)


def fused_body(n, nf, queries, corpus, candidates, threshold):
    rows_dev, width = corpus.shape
    owned, per_query = candidates.shape
    nq = n * owned
    capacity = (owned * per_query + n - 1) // n
    vmem = pl.BlockSpec(memory_space=pltpu.VMEM)
    mass, answers = pl.pallas_call(
        functools.partial(kernel, n, nf, rows_dev * n, capacity),
        out_shape=(
            jax.ShapeDtypeStruct((1, LANES), jnp.float32),
            jax.ShapeDtypeStruct((owned, LANES), jnp.float32),
        ),
        in_specs=[pl.BlockSpec(memory_space=pl.ANY)] * 4,
        out_specs=(vmem, vmem),
        scratch_shapes=[
            pltpu.VMEM(queries.shape, jnp.bfloat16),
            pltpu.VMEM((1, nq), jnp.int32),
            pltpu.VMEM((owned, per_query), jnp.int32),
            pltpu.VMEM((rows_dev, width), jnp.bfloat16),
            pltpu.VMEM((rows_dev, width), jnp.float32),
            pltpu.VMEM((owned, LANES), jnp.bfloat16),
            pltpu.VMEM((n, owned, LANES), jnp.bfloat16),
            pltpu.VMEM((nq, LANES), jnp.bfloat16),
            pltpu.VMEM((nq // TILE, LANES, TILE), jnp.bfloat16),
            pltpu.VMEM((owned, LANES), jnp.int32),
            pltpu.VMEM((LANES, owned * LANES), jnp.bfloat16),
            pltpu.VMEM((n, 1, LANES), jnp.int32),
            pltpu.VMEM((n, 1, LANES), jnp.int32),
            pltpu.VMEM((n, 1, LANES), jnp.int32),
            pltpu.SMEM((n, 1, LANES), jnp.int32),
            pltpu.VMEM((n, LANES, LANES), jnp.float32),
            pltpu.VMEM((n, 1, LANES), jnp.float32),
            pltpu.VMEM((n, 1, LANES), jnp.float32),
            pltpu.VMEM((nq // LANES, 1, LANES), jnp.float32),
            pltpu.VMEM((n, 1, LANES), jnp.float32),
            pltpu.SemaphoreType.DMA((3,)),
            pltpu.SemaphoreType.DMA,
            pltpu.SemaphoreType.DMA,
            pltpu.SemaphoreType.DMA,
            pltpu.SemaphoreType.DMA((nq // TILE,)),
            pltpu.SemaphoreType.DMA,
            pltpu.SemaphoreType.DMA((nq // TILE,)),
            pltpu.SemaphoreType.REGULAR,
            pltpu.SemaphoreType.DMA,
            pltpu.SemaphoreType.DMA,
            pltpu.SemaphoreType.DMA,
            pltpu.SemaphoreType.DMA,
            pltpu.SemaphoreType.DMA,
            pltpu.SemaphoreType.DMA,
        ],
        compiler_params=pltpu.CompilerParams(
            collective_id=0, has_side_effects=True),
    )(queries, threshold.reshape(1, nq), candidates, corpus)
    return mass[0, :owned], answers[:, :per_query]


def plain_body(queries, corpus, candidates, threshold):
    rows_dev = corpus.shape[0]
    width = corpus.shape[1]
    shards = lax.axis_size("rows") * lax.axis_size("feat")
    owned_queries = candidates.shape[0]
    per_query = candidates.shape[1]
    npass_all = rows_dev * shards
    cutoff = threshold.astype(jnp.float32) * 0.01
    owner = lax.axis_index(("rows", "feat"))
    full_rows = lax.all_gather(queries, "feat", axis=1, tiled=True)
    whole = lax.all_gather(full_rows, "rows", axis=0, tiled=True)
    query_count = whole.shape[0]
    block = 2048
    corpus_blocks = corpus.reshape(rows_dev // block, block, width)

    def visit(total, block_rows):
        scores = lax.dot_general(
            whole, block_rows, (((1,), (1,)), ((), ())), preferred_element_type=jnp.float32
        )
        return (total + jnp.sum(jnp.maximum(scores - cutoff[:, None], 0.0), axis=1), None)

    total, _ = lax.scan(visit, jnp.zeros((query_count,), jnp.float32), corpus_blocks)
    flat_ids = candidates.reshape(-1)
    total_ids = flat_ids.shape[0]
    capacity = (total_ids + shards - 1) // shards
    target = flat_ids // rows_dev
    onehot = (target[:, None] == jnp.arange(shards, dtype=jnp.int32)[None, :]).astype(jnp.int32)
    before = jnp.cumsum(onehot, axis=0) - onehot
    rank = jnp.sum(before * onehot, axis=1)
    query_ids = owner * owned_queries + jnp.arange(total_ids, dtype=jnp.int32) // per_query
    fields = jnp.stack([flat_ids - target * rows_dev, query_ids], axis=1)
    send_both = jnp.zeros((shards, capacity, 2), jnp.int32).at[target, rank].set(fields)
    n_rows = lax.axis_size("rows")
    n_feat = lax.axis_size("feat")
    received = lax.all_to_all(
        lax.all_to_all(
            send_both.reshape(n_rows, n_feat, capacity * 2),
            "rows",
            split_axis=0,
            concat_axis=0,
            tiled=True,
        ),
        "feat",
        split_axis=1,
        concat_axis=1,
        tiled=True,
    )
    received = received.reshape(shards * capacity, 2)
    picked = corpus[received[:, 0]]
    asked = whole[received[:, 1]]
    values = jnp.einsum("kd,kd->k", picked, asked, preferred_element_type=jnp.float32).reshape(
        n_rows, n_feat, capacity
    )
    partials = total.reshape(n_rows, n_feat, owned_queries)
    answers, mass_parts = (
        lax.all_to_all(
            lax.all_to_all(values, "rows", split_axis=0, concat_axis=0, tiled=True),
            "feat",
            split_axis=1,
            concat_axis=1,
            tiled=True,
        ),
        lax.all_to_all(
            lax.all_to_all(partials, "rows", split_axis=0, concat_axis=0, tiled=True),
            "feat",
            split_axis=1,
            concat_axis=1,
            tiled=True,
        ),
    )
    exceed = jnp.sum(mass_parts, axis=(0, 1)) * (8.0 / npass_all)
    candidate_scores = answers.reshape(shards, capacity)[target, rank].reshape(
        owned_queries, per_query
    )
    return (exceed, candidate_scores)


def body(queries, corpus, candidates, threshold):
    nf = lax.axis_size("feat")
    n = lax.axis_size("rows") * nf
    rows_dev, width = corpus.shape
    owned, per_query = candidates.shape
    capacity = (owned * per_query + n - 1) // n
    fits = (
        nf == 2
        and width == LANES
        and queries.shape == (2 * owned, LANES // 2)
        and owned % 32 == 0
        and LANES % owned == 0
        and per_query <= LANES
        and capacity <= LANES
        and n % 8 == 0
        and (n * owned) % TILE == 0
        and n * owned == 4 * TILE
        and rows_dev % BLOCK == 0
        and n % (rows_dev // MIXED) == 0
        and rows_dev % (2 * BLOCK) == 0
        and rows_dev & (rows_dev - 1) == 0
    )
    if fits:
        return fused_body(n, nf, queries, corpus, candidates, threshold)
    return plain_body(queries, corpus, candidates, threshold)


def solution(mesh):
    return jax.shard_map(
        body,
        mesh=mesh,
        in_specs=(P("rows", "feat"), P(("rows", "feat"), None), P(("rows", "feat"), None), P()),
        out_specs=(P(("rows", "feat")), P(("rows", "feat"), None)),
        check_vma=False,
    )
```
